256 devices in a mesh: dom: 64 (over x_lo, z, y), orb: 4 (over x_hi, core).
Axes of the slice: x: 4 (x_hi: 2, x_lo: 2; x = x_hi * 2 + x_lo), y: 4, z: 8, core: 2. Of those that a mesh axis runs over, the one named last changes fastest.
Arguments:
- orbitals: bfloat16 [128, 4, 1024, 512], P('dom', None, None, 'orb'), may hold values from -6 to 6
- slot_ids: int32 [128, 4], P('dom'), may hold values from 0 to 15, as said below
- slot_count: int32 [128], P('dom'), may hold values from 1 to 4, as said below
- band_tiles: bfloat16 [16, 3, 512, 512], P(None, None, 'dom', 'orb'), may hold values from -0.15625 to 0.15625
- pattern: int32 [16, 3], replicated, may hold values 0 or 1
- occupation: float32 [16, 512], P(None, 'orb'), may hold values from 0.0005 to 0.005
Outputs:
- rotated: bfloat16 [128, 4, 1024, 512], P('dom', None, None, 'orb')
- density: float32 [128, 1024], P('dom')
The draws below stay inside these ranges and needn't reach their ends.
Inputs may be any that keep to these rules, and one draw needn't show every extreme that they name: `slot_ids`: each row names 4 consecutive orbital blocks counted modulo 16: slot l holds (s + l) mod 16, where the first block s of a grid block may be any of the 16 blocks. The slots in use on grid block g are its first slot_count[g]; some grid block uses all 4.
All inputs are finite; a program needn't handle non-finite values.
Results may differ from the reference program's by a relative error of at most 0.00094.
Values may be sent and summed in bfloat16 or wider, within the bound.
A program may use at most 128 MiB of HBM per device.

```python
import math
import jax
import jax.numpy as jnp
from jax import lax

NB = 16
OB = 512
BAND = 3
L = 4
P_SIZE = 1024
G = 128


def draw_slot_ids(key, part):
    lowest = jax.random.randint(jax.random.fold_in(key, 11), (G,), 0, NB, dtype=jnp.int32)
    return ((lowest[:, None] + jnp.arange(L, dtype=jnp.int32)[None, :]) % NB).astype(jnp.int32)


def draw_slot_count(key, part):
    first_draw = jax.random.randint(jax.random.fold_in(key, 21), (G,), 0, L, dtype=jnp.int32)
    second = jax.random.randint(jax.random.fold_in(key, 22), (G,), 0, 2, dtype=jnp.int32)
    in_use = 1 + first_draw * second
    return jnp.where(jnp.arange(G, dtype=jnp.int32) == 0, L, in_use).astype(jnp.int32)


def touch_ends(drawn, key, least, largest):
    longest = drawn.shape.index(max(drawn.shape))
    spots = []
    for shift in (0, 1):
        where = [jax.random.randint(jax.random.fold_in(key, axis), (), 0, length) for axis, length in enumerate(drawn.shape)]
        where[longest] = (where[longest] + shift) % drawn.shape[longest]
        spots.append(tuple(where))
    return drawn.at[spots[0]].set(least).at[spots[1]].set(largest)


def shard_levels(key, dims, pieces, least, top_value):
    loudness = 1.0
    for position, parts in pieces:
        draws = jax.random.uniform(jax.random.fold_in(jax.random.fold_in(key, 6), position), (parts,), jnp.float32, least / len(pieces), top_value / len(pieces))
        loudness = loudness * jnp.repeat(jnp.exp(draws), dims[position] // parts).reshape((-1,) + (1,) * (len(dims) - 1 - position))
    return loudness


def normal_values(stream_key, dims, deviation, reach, pieces=(), kind=jnp.bfloat16):
    values = deviation * jax.random.normal(stream_key, dims, jnp.float32)
    if pieces:
        values = values * shard_levels(stream_key, dims, pieces, -0.22, 0.18)
    return jnp.clip(values, -reach, reach).astype(kind)


def setup_inputs(seed: int = 0) -> dict:
    key_list = jax.random.split(jax.random.key(seed), 7)
    return {
        "orbitals": normal_values(key_list[0], (G, L, P_SIZE, OB), 1.0, 6.0, ((0, 64), (3, 4))),
        "slot_ids": draw_slot_ids(jax.random.fold_in(key_list[6], 71), 0),
        "slot_count": draw_slot_count(jax.random.fold_in(key_list[6], 71), 0),
        "band_tiles": normal_values(key_list[3], (NB, BAND, OB, OB), (OB * BAND) ** -0.5, 0.15625, ((2, 64), (3, 4))),
        "pattern": touch_ends((jax.random.randint(key_list[4], (NB, BAND), 0, 4) < 3).astype(jnp.int32), jax.random.fold_in(key_list[4], 1), 0, 1),
        "occupation": jnp.clip(jnp.exp(math.log(0.005) - 2.30258502 * jax.random.uniform(key_list[5], (NB, OB), jnp.float32) ** shard_levels(key_list[5], (NB, OB), ((1, 4),), -0.2, 0.2)), 0.0005, 0.005),
    }


def select_tiles(band_tiles, pattern, block_ids, block_count):
    slots_per = block_ids.shape[0]
    band_count = pattern.shape[1]
    half_band = (band_count - 1) // 2
    active = jnp.arange(slots_per, dtype=jnp.int32) < block_count
    source = block_ids[:, None]
    target = block_ids[None, :]
    offset = target - source + half_band
    inside = (offset >= 0) & (offset < band_count)
    column = jnp.clip(offset, 0, band_count - 1).astype(jnp.int32)
    keeping = inside & (pattern[source, column] == 1) & active[:, None] & active[None, :]
    picked = band_tiles[source, column]
    return jnp.where(keeping[:, :, None, None], picked, jnp.zeros((), picked.dtype))


def reference(orbitals, slot_ids, slot_count, band_tiles, pattern, occupation):
    def one_block(block_items):
        values, block_ids, block_count = block_items
        tile_set = select_tiles(band_tiles, pattern, block_ids, block_count)
        rotated = jnp.einsum('lpi,lmij->mpj', values.astype(jnp.float32), tile_set.astype(jnp.float32), precision=lax.Precision.HIGHEST).astype(jnp.bfloat16)
        weights = occupation[block_ids]
        square = rotated.astype(jnp.float32) * rotated.astype(jnp.float32)
        density = jnp.einsum('mpj,mj->p', square, weights, precision=lax.Precision.HIGHEST)
        return rotated, density

    rotated, density = lax.map(one_block, (orbitals, slot_ids, slot_count))
    return (rotated, density)
```

```python
import heapq

import jax
import jax.numpy as jnp
from jax import lax
from jax.experimental import pallas as pl
from jax.experimental.pallas import tpu as pltpu
from jax.sharding import PartitionSpec as P

MESH = pl.DeviceIdType.MESH
NX, NY, NZ = 4, 4, 8
TILES = 46
A_TILES = 19
CHUNKS = 8
ROWS = 256
HALF = 128
B_SETS = {1: (0, 1, -2, 3), -1: (-1, 2, -3, 4)}


def messages():
    tile = 8 * 128 * 2
    a, b = A_TILES * tile, (TILES - A_TILES) * tile
    out = {}
    out["swap",] = ("xs", a + b, [("tiles",)])
    mine = [("swap",), ("tiles",)]
    for n in range(1, 5):
        for s in (1, -1):
            out["Bz", s, n] = (("z", s), 2 * b if n < 4 else b, mine if n == 1 else [("Bz", s, n - 1)])
    for s in (1, -1):
        out["Ay1", s] = (("y", s), 2 * a, mine)
        out["Ay2", s] = (("y", s), a, [("Ay1", s)])
    have_a = {0: mine, -1: [("Ay1", 1)], 1: [("Ay1", -1)], 2: [("Ay2", 1), ("Ay2", -1)]}
    for dy in (0, -1, 1, 2):
        for n in range(1, 5):
            for s in (1, -1):
                out["Az", s, dy, n] = (("z", s), 2 * a if n < 4 else a, have_a[dy] if n == 1 else [("Az", s, dy, n - 1)])
    have_b = {0: mine, 4: [("Bz", 1, 4), ("Bz", -1, 4)]}
    for n in range(1, 4):
        have_b[-n], have_b[n] = [("Bz", 1, n)], [("Bz", -1, n)]
    for dz in (0, -1, 1, -2, 2, -3, 3, 4):
        for s in (1, -1):
            out["By1", s, dz] = (("y", s), 2 * b, have_b[dz])
            if dz in B_SETS[s]:
                out["By2", s, dz] = (("y", s), 2 * b, [("By1", s, dz)])
    piece = 4 * HALF * 128 * 2
    for k in range(CHUNKS):
        for s in (1, -1):
            out["X1", s, k] = (("x", s), piece, [("own", k)])
    for k in range(CHUNKS):
        for s in (1, -1):
            out["X2", s, k] = (("x", s), piece, [("X1", s, k)])
            out["Xd", s, k] = ("d", piece, [("X2", s, k)])
        out["Od", k] = ("d", 2 * piece, [("own", k)])
    return out


def is_tile(key):
    return key[0] in ("swap", "Bz", "Ay1", "Ay2", "Az", "By1", "By2")


def plan():
    todo = messages()
    rate = {"xs": 46.6e3, "d": 330e3}
    free, here, due, order = {}, set(), [], []
    now = 0.0
    pending = dict(todo)

    def send_ready():
        for key in [k for k, v in pending.items() if all(need in here for need in v[2])]:
            link, size, _ = pending.pop(key)
            links = [("x", 1), ("x", -1)] if link == "xs" else [link]
            start = max([now] + [free.get(one, 0.0) for one in links])
            end = start + size / rate.get(link, 46.6e3)
            for one in links:
                free[one] = end
            heapq.heappush(due, (end + (1.1 if link == "d" else 1.9), len(order), key))
            order.append(("send", key))

    heapq.heappush(due, (0.4, -100, ("tiles",)))
    for k in range(CHUNKS):
        heapq.heappush(due, (0.5 + 0.1 * k, k - 50, ("own", k)))
    tiles_left = {key for key in todo if is_tile(key)} | {("tiles",)}
    weights, done = False, 0
    while due or done < CHUNKS:
        if due and due[0][0] <= now:
            key = heapq.heappop(due)[2]
            order.append(("wait", key))
            here.add(key)
            tiles_left.discard(key)
            send_ready()
            continue
        k = done
        ready = weights and k < CHUNKS and all(
            need in here for need in [("own", k), ("Od", k)] + [(t, s, k) for t in ("X2", "Xd") for s in (1, -1)]
        )
        if not weights and not tiles_left:
            order.append(("weights",))
            weights = True
            now += 1.5
        elif ready:
            order.append(("product", k))
            done += 1
            now += 0.6
        else:
            now = due[0][0]
    return order, now


def kernel(ids, count, pattern, band, orbitals, occ, rotated, density, T, X, F, W, O, dens, recv, sent, local, put, dsend, drecv):
    dom, orb = lax.axis_index("dom"), lax.axis_index("orb")
    x_lo, z, y = lax.div(dom, 32), lax.rem(lax.div(dom, 4), 8), lax.rem(dom, 4)
    x_hi, core = lax.div(orb, 2), lax.rem(orb, 2)
    x = x_hi * 2 + x_lo

    def at_x(step):
        return lax.rem(x + step + NX, NX)

    def at_y(step):
        return lax.rem(y + step + NY, NY)

    def at_z(step):
        return lax.rem(z + step + NZ, NZ)

    def device(px, py, pz, pc):
        return (lax.rem(px, 2) * 32 + pz * 4 + py, lax.div(px, 2) * 2 + pc)

    def orb_of(px):
        return lax.div(px, 2) * 2 + core

    swap_x = x + 1 - 2 * x_lo
    to = {
        "xs": device(swap_x, y, z, core),
        "d": device(x, y, z, 1 - core),
        "far": device(at_x(2), y, z, core),
        "cross": device(at_x(2), y, z, 1 - core),
    }
    for s in (1, -1):
        to["x", s] = device(at_x(s), y, z, core)
        to["y", s] = device(x, at_y(s), z, core)
        to["z", s] = device(x, y, at_z(s), core)

    def part(which):
        return pl.ds(0, A_TILES) if which == "A" else pl.ds(A_TILES, TILES - A_TILES)

    def lows(s, half):
        return pl.ds(0 if s > 0 else 1, 1) if half else pl.ds(0, 2)

    def piece(k, s):
        return pl.ds(k // 4 * 4, 4), pl.ds(k % 4 * ROWS + (0 if s > 0 else HALF), HALF)

    todo = messages()
    number = {key: i for i, key in enumerate(todo)}

    def copy(key):
        kind = key[0]
        if kind == "swap":
            src = dst = T.at[z, y, x_lo]
        elif kind == "Bz":
            _, s, n = key
            src = dst = T.at[at_z(-(n - 1) * s), y, lows(s, n == 4), part("B")]
        elif kind == "Ay1":
            src = dst = T.at[z, y, lows(1, False), part("A")]
        elif kind == "Ay2":
            src = dst = T.at[z, at_y(-key[1]), lows(key[1], True), part("A")]
        elif kind == "Az":
            _, s, dy, n = key
            src = dst = T.at[at_z(-(n - 1) * s), at_y(dy), lows(s, n == 4), part("A")]
        elif kind == "By1":
            src = dst = T.at[at_z(key[2]), y, lows(1, False), part("B")]
        elif kind == "By2":
            src = dst = T.at[at_z(key[2]), at_y(-key[1]), lows(1, False), part("B")]
        elif kind == "X1":
            _, s, k = key
            slots, rows = piece(k, s)
            src, dst = X.at[orb, slots, rows], F.at[0 if s > 0 else 1, k]
        elif kind == "X2":
            _, s, k = key
            slots, rows = piece(k, s)
            src, dst = F.at[0 if s > 0 else 1, k], X.at[orb_of(at_x(-s)), slots, rows]
        elif kind == "Xd":
            _, s, k = key
            slots, rows = piece(k, s)
            src = dst = X.at[orb_of(at_x(2)), slots, rows]
        else:
            k = key[1]
            src = dst = X.at[orb, pl.ds(k // 4 * 4, 4), pl.ds(k % 4 * ROWS, ROWS)]
        i = number[key]
        return pltpu.make_async_remote_copy(
            src_ref=src, dst_ref=dst, send_sem=sent.at[i], recv_sem=recv.at[i], device_id=to[todo[key][0]], device_id_type=MESH
        )

    def load(key):
        if key[0] == "tiles":
            return pltpu.make_async_copy(band.at[pl.ds(1, TILES)], T.at[z, y, x_lo], local.at[CHUNKS])
        k = key[1]
        slots, rows = pl.ds(k // 4 * 4, 4), pl.ds(k % 4 * ROWS, ROWS)
        return pltpu.make_async_copy(orbitals.at[slots, rows], X.at[orb, slots, rows], local.at[k])

    def store(k):
        slots, rows = pl.ds(k // 4 * 4, 4), pl.ds(k % 4 * ROWS, ROWS)
        return pltpu.make_async_copy(O.at[slots, rows], rotated.at[slots, rows], put.at[k])

    def weights():
        for g in range(2):
            for pair in range(2):
                for at in range(3):
                    l = pair + at
                    for side in range(2):
                        m = pair * 2 + side
                        block = (g * 2 + pair, pl.ds(at * 512, 512), pl.ds(side * 128, 128))
                        if abs(l - m) > 1:
                            W[block] = jnp.zeros((512, 128), jnp.bfloat16)
                            continue
                        source, target = ids[g, l], ids[g, m]
                        column = target - source + 1
                        inside = (column >= 0) & (column < 3)
                        column = jnp.clip(column, 0, 2)
                        last = max(l, m)
                        keep = inside & (pattern[source, column] == 1) & (last < count[g])
                        t = jnp.clip(source * 3 + column - 1, 0, TILES - 1)
                        scale = jnp.where(keep, jnp.float32(1), jnp.float32(0))
                        for low in range(2):
                            rows = T[:, :, low, t].astype(jnp.float32).reshape(256, 128) * scale
                            W[g * 2 + pair, pl.ds(at * 512 + low * 256, 256), pl.ds(side * 128, 128)] = rows.astype(jnp.bfloat16)

    def product(k):
        g, base = k // 4, k % 4 * ROWS
        rows = pl.ds(base, ROWS)
        total = jnp.zeros((ROWS, 128), jnp.float32)
        for pair in range(2):
            values = jnp.concatenate([X[q, g * 4 + pair + at, rows] for at in range(3) for q in range(4)], axis=1)
            out = jnp.dot(values, W[g * 2 + pair], preferred_element_type=jnp.float32).astype(jnp.bfloat16)
            for side in range(2):
                m = pair * 2 + side
                one = out[:, side * 128 : side * 128 + 128]
                O[g * 4 + m, rows] = one
                wide = one.astype(jnp.float32)
                total = total + wide * wide * occ[pl.ds(ids[g, m], 1), :]
        summed = lax.dot_general(
            jnp.ones((8, 128), jnp.float32), total, (((1,), (1,)), ((), ())),
            precision=lax.Precision.HIGHEST, preferred_element_type=jnp.float32,
        )
        dens[orb, pl.ds(g, 1), rows] = summed[0:1]
        store(k).start()

    load(("tiles",)).start()
    for k in range(CHUNKS):
        load(("own", k)).start()
    barrier = pltpu.get_barrier_semaphore()
    for peer in to:
        if peer != "xs":
            pl.semaphore_signal(barrier, inc=1, device_id=to[peer], device_id_type=MESH)
    pl.semaphore_wait(barrier, len(to) - 1)

    for step in plan()[0]:
        if step[0] == "send":
            copy(step[1]).start()
        elif step[0] == "wait":
            if step[1][0] in ("tiles", "own"):
                load(step[1]).wait()
            else:
                copy(step[1]).wait_recv()
        elif step[0] == "weights":
            weights()
        else:
            product(step[1])

    for key in todo:
        copy(key).wait_send()
    shares = [
        pltpu.make_async_remote_copy(
            src_ref=dens.at[orb], dst_ref=dens.at[orb], send_sem=dsend.at[i], recv_sem=drecv.at[i], device_id=to[peer], device_id_type=MESH
        )
        for i, peer in enumerate(("d", "far", "cross"))
    ]
    for share in shares:
        share.start()
    for k in range(CHUNKS):
        store(k).wait()
    for share in shares:
        share.wait_recv()
    density[...] = dens[0] + dens[1] + dens[2] + dens[3]
    for share in shares:
        share.wait_send()


def local(orbitals, slot_ids, slot_count, band_tiles, pattern, occupation):
    smem, hbm, vmem = (pl.BlockSpec(memory_space=s) for s in (pltpu.SMEM, pl.ANY, pltpu.VMEM))
    n = len(messages())
    rotated, density = pl.pallas_call(
        kernel,
        out_shape=(jax.ShapeDtypeStruct((8, 1024, 128), jnp.bfloat16), jax.ShapeDtypeStruct((2, 1024), jnp.float32)),
        in_specs=[smem, smem, smem, hbm, hbm, vmem],
        out_specs=(hbm, vmem),
        scratch_shapes=[
            pltpu.VMEM((NZ, NY, 2, TILES, 8, 128), jnp.bfloat16),
            pltpu.VMEM((4, 8, 1024, 128), jnp.bfloat16),
            pltpu.VMEM((2, CHUNKS, 4, HALF, 128), jnp.bfloat16),
            pltpu.VMEM((4, 1536, 256), jnp.bfloat16),
            pltpu.VMEM((8, 1024, 128), jnp.bfloat16),
            pltpu.VMEM((4, 2, 1024), jnp.float32),
            pltpu.SemaphoreType.DMA((n,)),
            pltpu.SemaphoreType.DMA((n,)),
            pltpu.SemaphoreType.DMA((CHUNKS + 1,)),
            pltpu.SemaphoreType.DMA((CHUNKS,)),
            pltpu.SemaphoreType.DMA((3,)),
            pltpu.SemaphoreType.DMA((3,)),
        ],
        compiler_params=pltpu.CompilerParams(collective_id=0, has_side_effects=True, vmem_limit_bytes=48 * 1024 * 1024),
    )(slot_ids, slot_count, pattern, band_tiles.reshape(48, 8, 128), orbitals.reshape(8, 1024, 128), occupation)
    return rotated.reshape(2, 4, 1024, 128), density


def solution(mesh):
    return jax.shard_map(
        local,
        mesh=mesh,
        in_specs=(
            P("dom", None, None, "orb"),
            P("dom", None),
            P("dom"),
            P(None, None, "dom", "orb"),
            P(),
            P(None, "orb"),
        ),
        out_specs=(P("dom", None, None, "orb"), P("dom", None)),
        check_vma=False,
    )
```

```python
import functools
import heapq

import jax
import jax.numpy as jnp
from jax import lax
from jax.experimental import pallas as pl
from jax.experimental.pallas import tpu as pltpu
from jax.sharding import PartitionSpec as P

MESH = pl.DeviceIdType.MESH
NX, NY, NZ = 4, 4, 8
TILES = 46
A_TILES = 18
VMEM_BYTES = 67043328 - 2097152 - 8192
B_SETS = {1: (0, 1, -2, 3), -1: (-1, 2, -3, 4)}
CHUNKS = [(0, a, 128) for a in range(0, 512, 128)] + [(1, 0, 128), (1, 128, 128), (1, 256, 128), (1, 384, 64), (1, 448, 32), (1, 480, 32)]
UNITS = [(0, 0, 256), (0, 256, 256), (1, 0, 256), (1, 256, 128), (1, 384, 64), (1, 448, 32), (1, 480, 32)]
TAIL = 384
DEPTH = 2


def messages():
    tile = 8 * 128 * 2
    a, b = A_TILES * tile, (TILES - A_TILES) * tile
    out = {}

    def add(key, link, size, needs, group=None):
        out[key] = (link, size, needs, group or key)

    add(("swap",), "xs", a + b, [("tiles",)])
    mine = [("swap",), ("z",)]
    for n in range(1, 5):
        for s in (1, -1):
            add(("Bz", s, n), ("z", s), 2 * b if n < 4 else b, mine if n == 1 else [("Bz", s, n - 1)], ("Bz4",) if n == 4 else None)
    for s in (1, -1):
        add(("Ay1", s), ("y", s), 2 * a, mine)
        add(("Ay2", s), ("y", s), a, [("Ay1", s)], ("Ay2",))
    have_a = {0: mine, -1: [("Ay1", 1)], 1: [("Ay1", -1)], 2: [("Ay2",)]}
    for dy in (0, -1, 1, 2):
        for n in range(1, 5):
            for s in (1, -1):
                needs = have_a[dy] if n == 1 else [("Az", s, dy, n - 1)]
                add(("Az", s, dy, n), ("z", s), 2 * a if n < 4 else a, needs, ("Az4",) if n == 4 else None)
    have_b = {0: mine, 4: [("Bz4",)]}
    for n in range(1, 4):
        have_b[-n], have_b[n] = [("Bz", 1, n)], [("Bz", -1, n)]
    for dz in (0, -1, 1, -2, 2, -3, 3, 4):
        for s in (1, -1):
            onward = dz in B_SETS[s]
            add(("By1", s, dz), ("y", s), 2 * b, have_b[dz], None if onward else ("By1", s))
            if onward:
                add(("By2", s, dz), ("y", s), 2 * b, [("By1", s, dz)], ("By2",))
    row = 4 * 128 * 2
    for i in range(4):
        for s in (1, -1):
            add(("X1", s, i), ("x", s), 256 * row, [("own", i // 2)])
    for g in range(2):
        add(("Od", g), "d", 1024 * row, [("own", g)])
    for k, (g, first, rows) in enumerate(CHUNKS):
        for s in (1, -1):
            add(("X2", s, k), ("x", s), rows * row, [("X1", s, g * 2 + first // 256)], ("X2", k))
        add(("Xd", k), "d", 2 * rows * row, [("X2", k)])
    return out


def plan():
    todo = messages()
    rate = {"d": 690e3}
    left, after = {}, {}
    for key, (_, _, needs, group) in todo.items():
        left.setdefault(group, set()).add(key)
        for need in needs:
            after.setdefault(need, []).append(key)

    @functools.lru_cache(None)
    def path(key):
        link, size, _, group = todo[key]
        return size / rate.get(link, 45e3) + 1.9 + max([path(k) for k in after.get(group, [])], default=0)

    free, here, due, order, pending = {}, set(), [], [], dict(todo)
    now = 0.0

    def send_ready():
        ready = [k for k, v in pending.items() if all(need in here for need in v[2])]
        for key in sorted(ready, key=lambda k: -path(k) if k[0][0] in "AB" else 0):
            link, size, _, group = todo[key]
            busy = [t for t in free.get(link, []) if t > now]
            if link[0] in "yz" and len(busy) >= DEPTH:
                continue
            pending.pop(key)
            links = [("x", 1), ("x", -1)] if link == "xs" else [link]
            start = max([now] + [t for one in links for t in free.get(one, [])[-1:]])
            end = start + size / rate.get(link, 45e3)
            for one in links:
                free.setdefault(one, []).append(end)
            heapq.heappush(due, (end + (1.0 if link == "d" else 1.9), len(order), key))
            order.append(("send", key))

    for i, group in enumerate([("tiles",), ("own", 0), ("own", 1), ("z",)]):
        heapq.heappush(due, (0.01 * i, i - 50, group))
        left[group] = {group}
    tiles_left = {g for g in left if g[0] in ("tiles", "swap", "Bz", "Bz4", "Ay1", "Ay2", "Az", "Az4", "By1", "By2")}
    weights, done = False, 0
    while due or done < len(UNITS):
        if due and due[0][0] <= now:
            key = heapq.heappop(due)[2]
            group = todo[key][3] if key in todo else key
            left[group].discard(key)
            if not left[group]:
                order.append(("wait", group))
                here.add(group)
                tiles_left.discard(group)
            send_ready()
            continue
        ready = False
        if weights and done < len(UNITS):
            g, first, rows = UNITS[done]
            parts = [k for k, (cg, ca, _) in enumerate(CHUNKS) if cg == g and first <= ca < first + rows]
            ready = ("Od", g) in here and all((t, k) in here for t in ("X2", "Xd") for k in parts)
        if not weights and not tiles_left:
            order.append(("weights",))
            weights = True
            now += 0.7
        elif ready:
            order.append(("product", done))
            now += 0.4 + 0.4 * UNITS[done][2] / 128
            done += 1
        else:
            now = due[0][0]
    assert not pending
    return order, now


def kernel(
    ids_in, count_in, pattern_in, band, orbitals, occ_in, rotated, density,
    ids, count, pattern, occ, T, X, F, W, D, dens, recv, sent, local, small, shared, ready,
):
    dom, orb = lax.axis_index("dom"), lax.axis_index("orb")
    x_lo, z, y = lax.div(dom, 32), lax.rem(lax.div(dom, 4), 8), lax.rem(dom, 4)
    x_hi, core = lax.div(orb, 2), lax.rem(orb, 2)
    x = x_hi * 2 + x_lo

    def at_x(step):
        return lax.rem(x + step + NX, NX)

    def at_y(step):
        return lax.rem(y + step + NY, NY)

    def at_z(step):
        return lax.rem(z + step + NZ, NZ)

    def device(px, py, pz, pc):
        return (lax.rem(px, 2) * 32 + pz * 4 + py, lax.div(px, 2) * 2 + pc)

    far = lax.div(at_x(2), 2) * 2 + core
    to = {"xs": device(x + 1 - 2 * x_lo, y, z, core), "d": device(x, y, z, 1 - core)}
    for s in (1, -1):
        to["x", s] = device(at_x(s), y, z, core)
        to["y", s] = device(x, at_y(s), z, core)
        to["z", s] = device(x, y, at_z(s), core)

    A, B, BOTH, ALL = pl.ds(0, A_TILES), pl.ds(A_TILES, TILES - A_TILES), pl.ds(0, 2), slice(None)

    def lows(s, half):
        return pl.ds(0 if s > 0 else 1, 1) if half else BOTH

    def side(s):
        return 0 if s > 0 else 1

    todo = messages()
    groups = list(dict.fromkeys(v[3] for v in todo.values()))
    number = {group: i for i, group in enumerate(groups)}

    def ends(key):
        kind = key[0]
        if kind == "swap":
            return (T.at[z, y, x_lo],) * 2
        if kind == "Bz":
            _, s, n = key
            return (T.at[at_z(-(n - 1) * s), y, lows(s, n == 4), B],) * 2
        if kind == "Ay1":
            return (T.at[z, y, BOTH, A],) * 2
        if kind == "Ay2":
            return (T.at[z, at_y(-key[1]), lows(key[1], True), A],) * 2
        if kind == "Az":
            _, s, dy, n = key
            return (T.at[at_z(-(n - 1) * s), at_y(dy), lows(s, n == 4), A],) * 2
        if kind == "By1":
            return (T.at[at_z(key[2]), y, BOTH, B],) * 2
        if kind == "By2":
            return (T.at[at_z(key[2]), at_y(-key[1]), BOTH, B],) * 2
        if kind == "X1":
            _, s, i = key
            rows = pl.ds(i % 2 * 256, 256)
            return X.at[orb, i // 2, ALL, side(s), rows], F.at[side(s), i // 2, ALL, rows]
        if kind == "X2":
            _, s, k = key
            g, first, rows = CHUNKS[k]
            source = lax.div(at_x(-s), 2) * 2 + core
            return F.at[side(s), g, ALL, pl.ds(first, rows)], X.at[source, g, ALL, side(s), pl.ds(first, rows)]
        if kind == "Xd":
            g, first, rows = CHUNKS[key[1]]
            return (X.at[far, g, ALL, ALL, pl.ds(first, rows)],) * 2
        return (X.at[orb, key[1]],) * 2

    def copy(key):
        src, dst = ends(key)
        return pltpu.make_async_remote_copy(
            src_ref=src, dst_ref=dst, send_sem=sent.at[0], recv_sem=recv.at[number[todo[key][3]]],
            device_id=to[todo[key][0]], device_id_type=MESH,
        )

    def landed(group):
        kind = group[0]
        if kind == "Bz4":
            where = T.at[z, y, BOTH, B]
        elif kind == "Ay2":
            where = T.at[z, y, BOTH, A]
        elif kind == "Az4":
            where = T.at[z, ALL, BOTH, A]
        elif kind == "By1" and len(group) == 2:
            where = T.at[pl.ds(0, 4), y, BOTH, B]
        elif kind == "By2":
            where = T.at[ALL, y, BOTH, B]
        elif kind == "X2":
            g, first, rows = CHUNKS[group[1]]
            where = X.at[far, g, ALL, ALL, pl.ds(first, rows)]
        else:
            where = ends(group)[1]
        pltpu.make_async_copy(where, where, recv.at[number[group]]).wait()

    loads = {("tiles",): pltpu.make_async_copy(band.at[pl.ds(1, TILES)], T.at[z, y, x_lo], local.at[0])}
    for g in range(2):
        loads["own", g] = pltpu.make_async_copy(orbitals.at[g], X.at[orb, g], local.at[1 + g])
    tables = [
        pltpu.make_async_copy(here, there, small.at[i])
        for i, (here, there) in enumerate(((ids_in, ids), (count_in, count), (pattern_in, pattern), (occ_in, occ)))
    ]

    def weights():
        for g in range(2):
            for pair in range(2):
                for at in range(3):
                    l = pair + at
                    for half in range(2):
                        m = pair * 2 + half
                        columns = pl.ds(half * 128, 128)
                        if abs(l - m) > 1:
                            W[g * 2 + pair, pl.ds(at * 512, 512), columns] = jnp.zeros((512, 128), jnp.bfloat16)
                            continue
                        source, target = ids[g, l], ids[g, m]
                        column = target - source + 1
                        inside = (column >= 0) & (column < 3)
                        column = jnp.clip(column, 0, 2)
                        keep = inside & (pattern[column, source] == 1) & (max(l, m) < count[g])
                        t = jnp.clip(source * 3 + column - 1, 0, TILES - 1)
                        scale = jnp.where(keep, jnp.float32(1), jnp.float32(0))
                        for low in range(2):
                            rows = T[:, :, low, t].astype(jnp.float32).reshape(256, 128) * scale
                            W[g * 2 + pair, pl.ds(at * 512 + low * 256, 256), columns] = rows.astype(jnp.bfloat16)

    def lane_sums(total):
        high = total.astype(jnp.bfloat16)
        rest = total - high.astype(jnp.float32)
        middle = rest.astype(jnp.bfloat16)
        low = (rest - middle.astype(jnp.float32)).astype(jnp.bfloat16)
        return lax.dot_general(
            jnp.ones((8, 384), jnp.bfloat16), jnp.concatenate([high, middle, low], axis=1),
            (((1,), (1,)), ((), ())), preferred_element_type=jnp.float32,
        )

    def product(u):
        g, first, n = UNITS[u]
        rows = pl.ds(first, n)
        total = jnp.zeros((2 * n, 128), jnp.float32)
        for pair in range(2):
            values = jnp.concatenate(
                [
                    jnp.concatenate([X[q, g, pair + at, half, rows] for at in range(3) for q in range(4)], axis=1)
                    for half in range(2)
                ],
                axis=0,
            )
            out = jnp.dot(values, W[g * 2 + pair], preferred_element_type=jnp.float32).astype(jnp.bfloat16)
            for which in range(2):
                m = pair * 2 + which
                one = out[:, which * 128 : which * 128 + 128]
                for half in range(2):
                    rotated[g, m, half, rows] = one[half * n : half * n + n]
                wide = one.astype(jnp.float32)
                total = total + wide * wide * occ[pl.ds(ids[g, m], 1), :]
        tail = g == 1 and first >= TAIL
        if tail:
            for half in range(2):
                D[half, pl.ds(first - TAIL, n)] = total[half * n : half * n + n]
            if u < len(UNITS) - 1:
                return
            first, n = TAIL, 512 - TAIL
            total = D[...].reshape(2 * n, 128)
        summed = lane_sums(total)
        for half in range(2):
            dens[orb, pl.ds(g, 1), pl.ds(half * 512 + first, n)] = summed[0:1, half * n : half * n + n]

    for load in loads.values():
        load.start()
    for table in tables:
        table.start()

    barrier = pltpu.get_barrier_semaphore()
    for step in (1, -1, 2):
        pl.semaphore_signal(barrier, inc=1, device_id=device(at_x(step), y, z, 0), device_id_type=MESH)
    for step in (1, -1):
        pl.semaphore_signal(barrier, inc=1, device_id=device(x, at_y(step), z, 1), device_id_type=MESH)
        pl.semaphore_signal(barrier, inc=1, device_id=device(x, y, at_z(step), 1), device_id_type=MESH)

    @pl.when(core == 1)
    def _():
        pl.semaphore_signal(barrier, inc=1, device_id=device(x, y, z, 0), device_id_type=MESH)

    @pl.when(core == 0)
    def _():
        pl.semaphore_wait(barrier, 7)
        pl.semaphore_signal(ready, inc=1, device_id=device(x, y, z, 1), device_id_type=MESH)

    @pl.when(core == 1)
    def _():
        pl.semaphore_wait(ready, 1)

    def neighbours():
        @pl.when(core == 1)
        def _():
            pl.semaphore_wait(barrier, 8)
            pl.semaphore_signal(ready, inc=1, device_id=device(x, y, z, 0), device_id_type=MESH)

        @pl.when(core == 0)
        def _():
            pl.semaphore_wait(ready, 1)

    for step in plan()[0]:
        if step[0] == "send":
            copy(step[1]).start()
        elif step[0] == "product":
            product(step[1])
        elif step[0] == "weights":
            for table in tables:
                table.wait()
            weights()
        elif step[1] in loads:
            loads[step[1]].wait()
        elif step[1] == ("z",):
            neighbours()
        else:
            landed(step[1])

    for key in todo:
        copy(key).wait_send()
    shares = [
        pltpu.make_async_remote_copy(
            src_ref=dens.at[orb], dst_ref=dens.at[orb], send_sem=shared.at[0], recv_sem=shared.at[1], device_id=peer, device_id_type=MESH
        )
        for peer in (device(at_x(2), y, z, core), device(at_x(2), y, z, 1 - core), to["d"])
    ]
    for share in shares:
        share.start()
    three = dens.at[pl.ds(0, 3)]
    pltpu.make_async_copy(three, three, shared.at[1]).wait()
    density[...] = dens[0] + dens[1] + dens[2] + dens[3]
    pltpu.make_async_copy(three, three, shared.at[0]).wait()


def write_out(held, held_density, rotated, density, sem):
    copies = [pltpu.make_async_copy(held.at[g, m], rotated.at[g, m], sem.at[g * 4 + m]) for g in range(2) for m in range(4)]
    copies.append(pltpu.make_async_copy(held_density, density, sem.at[8]))
    for one in copies:
        one.start()
    for one in copies:
        one.wait()


def local(orbitals, slot_ids, slot_count, band_tiles, pattern, occupation):
    hbm, anywhere = (pl.BlockSpec(memory_space=s) for s in (pltpu.HBM, pl.ANY))
    n = len({v[3] for v in messages().values()})
    values, sums = ((2, 4, 2, 512, 128), jnp.bfloat16), ((2, 1024), jnp.float32)
    held = pl.pallas_call(
        kernel,
        out_shape=(pltpu.VMEM(*values), pltpu.VMEM(*sums)),
        in_specs=[hbm] * 6,
        scratch_shapes=[
            pltpu.SMEM((2, 4), jnp.int32),
            pltpu.SMEM((2,), jnp.int32),
            pltpu.SMEM((3, 16), jnp.int32),
            pltpu.VMEM((16, 128), jnp.float32),
            pltpu.VMEM((NZ, NY, 2, TILES, 8, 128), jnp.bfloat16),
            pltpu.VMEM((4, 2, 4, 2, 512, 128), jnp.bfloat16),
            pltpu.VMEM((2, 2, 4, 512, 128), jnp.bfloat16),
            pltpu.VMEM((4, 1536, 256), jnp.bfloat16),
            pltpu.VMEM((2, 512 - TAIL, 128), jnp.float32),
            pltpu.VMEM((4, 2, 1024), jnp.float32),
            pltpu.SemaphoreType.DMA((n,)),
            pltpu.SemaphoreType.DMA((1,)),
            pltpu.SemaphoreType.DMA((3,)),
            pltpu.SemaphoreType.DMA((4,)),
            pltpu.SemaphoreType.DMA((2,)),
            pltpu.SemaphoreType.REGULAR,
        ],
        compiler_params=pltpu.CompilerParams(collective_id=0, has_side_effects=True, vmem_limit_bytes=VMEM_BYTES),
    )(slot_ids, slot_count, pattern.T, band_tiles.reshape(48, 8, 128), orbitals.reshape(2, 4, 2, 512, 128), occupation)
    rotated, density = pl.pallas_call(
        write_out,
        out_shape=(jax.ShapeDtypeStruct(*values), jax.ShapeDtypeStruct(*sums)),
        in_specs=[anywhere] * 2,
        out_specs=(hbm, hbm),
        scratch_shapes=[pltpu.SemaphoreType.DMA((9,))],
        compiler_params=pltpu.CompilerParams(vmem_limit_bytes=1024 * 1024),
    )(*held)
    return rotated.reshape(2, 4, 1024, 128), density


def solution(mesh):
    return jax.shard_map(
        local,
        mesh=mesh,
        in_specs=(
            P("dom", None, None, "orb"),
            P("dom", None),
            P("dom"),
            P(None, None, "dom", "orb"),
            P(),
            P(None, "orb"),
        ),
        out_specs=(P("dom", None, None, "orb"), P("dom", None)),
        check_vma=False,
    )
```

```python
import functools
import heapq

import jax
import jax.numpy as jnp
from jax import lax
from jax.experimental import pallas as pl
from jax.experimental.pallas import tpu as pltpu
from jax.sharding import PartitionSpec as P

MESH = pl.DeviceIdType.MESH
NX, NY, NZ = 4, 4, 8
TILES = 46
A_TILES = 18
VMEM_BYTES = 67043328 - 2097152 - 8192
B_SETS = {1: (0, 1, -2, 3), -1: (-1, 2, -3, 4)}
CHUNKS = [(0, 0, 256), (0, 256, 256), (1, 0, 128), (1, 128, 128), (1, 256, 128), (1, 384, 64), (1, 448, 32), (1, 480, 32)]
UNITS = [(0, 0, 256), (0, 256, 256), (1, 0, 256), (1, 256, 128), (1, 384, 64), (1, 448, 32), (1, 480, 32)]
TAIL = 384
DEPTH = 2


def messages():
    tile = 8 * 128 * 2
    a, b = A_TILES * tile, (TILES - A_TILES) * tile
    out = {}

    def add(key, link, size, needs, group=None):
        out[key] = (link, size, needs, group or key)

    add(("swap",), "xs", a + b, [("tiles",)])
    mine = [("swap",), ("z",)]
    for n in range(1, 5):
        for s in (1, -1):
            add(("Bz", s, n), ("z", s), 2 * b if n < 4 else b, mine if n == 1 else [("Bz", s, n - 1)], ("Bz4",) if n == 4 else None)
    for s in (1, -1):
        add(("Ay1", s), ("y", s), 2 * a, mine, ("Ay1",))
        add(("Ay2", s), ("y", s), a, [("Ay1",)], ("Ay2",))
    have_a = {0: mine, -1: [("Ay1",)], 1: [("Ay1",)], 2: [("Ay2",)]}
    for dy in (0, -1, 1, 2):
        for n in range(1, 5):
            for s in (1, -1):
                needs = have_a[dy] if n == 1 else [("Az", s, dy, n - 1)]
                add(("Az", s, dy, n), ("z", s), 2 * a if n < 4 else a, needs, ("Az4",) if n == 4 else None)
    have_b = {0: mine, 4: [("Bz4",)]}
    for n in range(1, 4):
        have_b[-n], have_b[n] = [("Bz", 1, n)], [("Bz", -1, n)]
    for dz in (0, -1, 1, -2, 2, -3, 3, 4):
        for s in (1, -1):
            onward = dz in B_SETS[s]
            add(("By1", s, dz), ("y", s), 2 * b, have_b[dz], None if onward else ("By1", s))
            if onward:
                add(("By2", s, dz), ("y", s), 2 * b, [("By1", s, dz)], ("By2",))
    row = 4 * 128 * 2
    for i in range(4):
        for s in (1, -1):
            add(("X1", s, i), ("x", s), 256 * row, [("own", i // 2)], ("X1", i))
    add(("Od",), "d", 2048 * row, [("own", 0), ("own", 1)])
    for k, (g, first, rows) in enumerate(CHUNKS):
        for s in (1, -1):
            add(("X2", s, k), ("x", s), rows * row, [("X1", g * 2 + first // 256)], ("X2", k))
        add(("Xd", k), "d", 2 * rows * row, [("X2", k)])
    return out


def chunks_of(u):
    if u >= len(UNITS):
        return []
    g, first, rows = UNITS[u]
    return [k for k, (cg, ca, _) in enumerate(CHUNKS) if cg == g and first <= ca < first + rows]


def plan():
    todo = messages()
    rate = {"d": 690e3}
    left, after = {}, {}
    for key, (_, _, needs, group) in todo.items():
        left.setdefault(group, set()).add(key)
        for need in needs:
            after.setdefault(need, []).append(key)

    @functools.lru_cache(None)
    def path(key):
        link, size, _, group = todo[key]
        return size / rate.get(link, 45e3) + 1.9 + max([path(k) for k in after.get(group, [])], default=0)

    free, here, due, order, pending = {}, set(), [], [], dict(todo)
    now = 0.0

    def send_ready():
        ready = [k for k, v in pending.items() if all(need in here for need in v[2])]
        for key in sorted(ready, key=lambda k: -path(k) if k[0][0] in "AB" else 0):
            link, size, _, group = todo[key]
            busy = [t for t in free.get(link, []) if t > now]
            if link[0] in "yz" and len(busy) >= DEPTH:
                continue
            pending.pop(key)
            links = [("x", 1), ("x", -1)] if link == "xs" else [link]
            start = max([now] + [t for one in links for t in free.get(one, [])[-1:]])
            end = start + size / rate.get(link, 45e3)
            for one in links:
                free.setdefault(one, []).append(end)
            heapq.heappush(due, (end + (1.0 if link == "d" else 1.9), len(order), key))
            order.append(("send", key))

    for i, group in enumerate([("tiles",), ("own", 0), ("own", 1), ("z",)]):
        heapq.heappush(due, (3.0 if group == ("z",) else 0.01 * i, i - 50, group))
        left[group] = {group}
    tiles_left = {g for g in left if g[0] in ("tiles", "swap", "Bz", "Bz4", "Ay1", "Ay2", "Az", "Az4", "By1", "By2")}
    weights, done = False, 0
    while due or done < len(UNITS):
        if due and due[0][0] <= now:
            key = heapq.heappop(due)[2]
            group = todo[key][3] if key in todo else key
            left[group].discard(key)
            if not left[group]:
                order.append(("wait", group))
                here.add(group)
                tiles_left.discard(group)
            send_ready()
            continue
        ready = weights and done < len(UNITS) and ("Od",) in here
        if ready:
            ready = all((t, k) in here for t in ("X2", "Xd") for k in chunks_of(done)) and all(("X2", k) in here for k in chunks_of(done + 1))
        if not weights and not tiles_left:
            order.append(("weights",))
            weights = True
            now += 0.7
        elif ready:
            if UNITS[done][:2] == (1, TAIL):
                order.append(("share",))
            order.append(("product", done))
            now += 0.4 + 0.4 * UNITS[done][2] / 128
            done += 1
        else:
            now = due[0][0]
    assert not pending
    return order, now


def kernel(
    ids_in, count_in, pattern_in, band, orbitals, occ_in, rotated, density,
    ids, count, pattern, occ, T, X, F, W, D, dens, tails, recv, sent, local, shared, ready,
):
    dom, orb = lax.axis_index("dom"), lax.axis_index("orb")
    x_lo, z, y = lax.div(dom, 32), lax.rem(lax.div(dom, 4), 8), lax.rem(dom, 4)
    x_hi, core = lax.div(orb, 2), lax.rem(orb, 2)
    x = x_hi * 2 + x_lo

    def at_x(step):
        return lax.rem(x + step + NX, NX)

    def at_y(step):
        return lax.rem(y + step + NY, NY)

    def at_z(step):
        return lax.rem(z + step + NZ, NZ)

    def device(px, py, pz, pc):
        return (lax.rem(px, 2) * 32 + pz * 4 + py, lax.div(px, 2) * 2 + pc)

    far = lax.div(at_x(2), 2) * 2 + core
    to = {"xs": device(x + 1 - 2 * x_lo, y, z, core), "d": device(x, y, z, 1 - core)}
    for s in (1, -1):
        to["x", s] = device(at_x(s), y, z, core)
        to["y", s] = device(x, at_y(s), z, core)
        to["z", s] = device(x, y, at_z(s), core)

    A, B, BOTH, ALL = pl.ds(0, A_TILES), pl.ds(A_TILES, TILES - A_TILES), pl.ds(0, 2), slice(None)

    def lows(s, half):
        return pl.ds(0 if s > 0 else 1, 1) if half else BOTH

    def side(s):
        return 0 if s > 0 else 1

    todo = messages()
    groups = list(dict.fromkeys(v[3] for v in todo.values()))
    number = {group: i for i, group in enumerate(groups)}

    def ends(key):
        kind = key[0]
        if kind == "swap":
            return (T.at[z, y, x_lo],) * 2
        if kind == "Bz":
            _, s, n = key
            return (T.at[at_z(-(n - 1) * s), y, lows(s, n == 4), B],) * 2
        if kind == "Ay1":
            return (T.at[z, y, BOTH, A],) * 2
        if kind == "Ay2":
            return (T.at[z, at_y(-key[1]), lows(key[1], True), A],) * 2
        if kind == "Az":
            _, s, dy, n = key
            return (T.at[at_z(-(n - 1) * s), at_y(dy), lows(s, n == 4), A],) * 2
        if kind == "By1":
            return (T.at[at_z(key[2]), y, BOTH, B],) * 2
        if kind == "By2":
            return (T.at[at_z(key[2]), at_y(-key[1]), BOTH, B],) * 2
        if kind == "X1":
            _, s, i = key
            rows = pl.ds(i % 2 * 256, 256)
            return X.at[orb, i // 2, ALL, side(s), rows], F.at[side(s), i // 2, ALL, rows]
        if kind == "X2":
            _, s, k = key
            g, first, rows = CHUNKS[k]
            source = lax.div(at_x(-s), 2) * 2 + core
            return F.at[side(s), g, ALL, pl.ds(first, rows)], X.at[source, g, ALL, side(s), pl.ds(first, rows)]
        if kind == "Xd":
            g, first, rows = CHUNKS[key[1]]
            return (X.at[far, g, ALL, ALL, pl.ds(first, rows)],) * 2
        return (X.at[orb],) * 2

    def copy(key):
        src, dst = ends(key)
        return pltpu.make_async_remote_copy(
            src_ref=src, dst_ref=dst, send_sem=sent.at[0], recv_sem=recv.at[number[todo[key][3]]],
            device_id=to[todo[key][0]], device_id_type=MESH,
        )

    def landed(group):
        kind = group[0]
        if kind == "Bz4":
            where = T.at[z, y, BOTH, B]
        elif kind == "Ay1":
            where = T.at[z, pl.ds(0, 2), BOTH, A]
        elif kind == "Ay2":
            where = T.at[z, y, BOTH, A]
        elif kind == "X1":
            where = F.at[ALL, group[1] // 2, ALL, pl.ds(group[1] % 2 * 256, 256)]
        elif kind == "Az4":
            where = T.at[z, ALL, BOTH, A]
        elif kind == "By1" and len(group) == 2:
            where = T.at[pl.ds(0, 4), y, BOTH, B]
        elif kind == "By2":
            where = T.at[ALL, y, BOTH, B]
        elif kind == "X2":
            g, first, rows = CHUNKS[group[1]]
            where = X.at[far, g, ALL, ALL, pl.ds(first, rows)]
        else:
            where = ends(group)[1]
        pltpu.make_async_copy(where, where, recv.at[number[group]]).wait()

    loads = {("tiles",): pltpu.make_async_copy(band.at[pl.ds(1, TILES)], T.at[z, y, x_lo], local.at[0])}
    for g in range(2):
        loads["own", g] = pltpu.make_async_copy(orbitals.at[g], X.at[orb, g], local.at[1 + g])
    tables = [
        pltpu.make_async_copy(here, there, local.at[3])
        for here, there in ((ids_in, ids), (count_in, count), (pattern_in, pattern), (occ_in, occ))
    ]

    def weights():
        for g in range(2):
            for pair in range(2):
                for at in range(3):
                    l = pair + at
                    for half in range(2):
                        m = pair * 2 + half
                        columns = pl.ds(half * 128, 128)
                        if abs(l - m) > 1:
                            W[g * 2 + pair, pl.ds(at * 512, 512), columns] = jnp.zeros((512, 128), jnp.bfloat16)
                            continue
                        source, target = ids[g, l], ids[g, m]
                        column = target - source + 1
                        inside = (column >= 0) & (column < 3)
                        column = jnp.clip(column, 0, 2)
                        keep = inside & (pattern[column, source] == 1) & (max(l, m) < count[g])
                        t = jnp.clip(source * 3 + column - 1, 0, TILES - 1)
                        scale = jnp.where(keep, jnp.float32(1), jnp.float32(0))
                        for low in range(2):
                            rows = T[:, :, low, t].astype(jnp.float32).reshape(256, 128) * scale
                            W[g * 2 + pair, pl.ds(at * 512 + low * 256, 256), columns] = rows.astype(jnp.bfloat16)

    def lane_sums(total):
        high = total.astype(jnp.bfloat16)
        rest = total - high.astype(jnp.float32)
        middle = rest.astype(jnp.bfloat16)
        low = (rest - middle.astype(jnp.float32)).astype(jnp.bfloat16)
        return lax.dot_general(
            jnp.ones((8, 384), jnp.bfloat16), jnp.concatenate([high, middle, low], axis=1),
            (((1,), (1,)), ((), ())), preferred_element_type=jnp.float32,
        )

    def product(u):
        g, first, n = UNITS[u]
        rows = pl.ds(first, n)
        total = jnp.zeros((2 * n, 128), jnp.float32)
        for pair in range(2):
            values = jnp.concatenate(
                [
                    jnp.concatenate([X[q, g, pair + at, half, rows] for at in range(3) for q in range(4)], axis=1)
                    for half in range(2)
                ],
                axis=0,
            )
            out = jnp.dot(values, W[g * 2 + pair], preferred_element_type=jnp.float32).astype(jnp.bfloat16)
            for which in range(2):
                m = pair * 2 + which
                one = out[:, which * 128 : which * 128 + 128]
                for half in range(2):
                    rotated[g, m, half, rows] = one[half * n : half * n + n]
                wide = one.astype(jnp.float32)
                total = total + wide * wide * occ[pl.ds(ids[g, m], 1), :]
        tail = g == 1 and first >= TAIL
        if tail:
            for half in range(2):
                D[half, pl.ds(first - TAIL, n)] = total[half * n : half * n + n]
            if u < len(UNITS) - 1:
                return
            n = 512 - TAIL
            summed = lane_sums(D[...].reshape(2 * n, 128))
            for half in range(2):
                tails[orb, pl.ds(half, 1)] = summed[0:1, half * n : half * n + n]
            return
        summed = lane_sums(total)
        for half in range(2):
            dens[orb, pl.ds(g, 1), pl.ds(half * 512 + first, n)] = summed[0:1, half * n : half * n + n]

    for load in loads.values():
        load.start()
    for table in tables:
        table.start()

    barrier = pltpu.get_barrier_semaphore()
    for step in (1, -1, 2):
        pl.semaphore_signal(barrier, inc=1, device_id=device(at_x(step), y, z, 0), device_id_type=MESH)
    for step in (1, -1):
        pl.semaphore_signal(barrier, inc=1, device_id=device(x, at_y(step), z, 1), device_id_type=MESH)
        pl.semaphore_signal(barrier, inc=1, device_id=device(x, y, at_z(step), 1), device_id_type=MESH)

    @pl.when(core == 1)
    def _():
        pl.semaphore_signal(barrier, inc=1, device_id=device(x, y, z, 0), device_id_type=MESH)

    @pl.when(core == 0)
    def _():
        pl.semaphore_wait(barrier, 7)
        pl.semaphore_signal(ready, inc=1, device_id=device(x, y, z, 1), device_id_type=MESH)

    @pl.when(core == 1)
    def _():
        pl.semaphore_wait(ready, 1)

    def neighbours():
        @pl.when(core == 1)
        def _():
            pl.semaphore_wait(barrier, 8)
            pl.semaphore_signal(ready, inc=1, device_id=device(x, y, z, 0), device_id_type=MESH)

        @pl.when(core == 0)
        def _():
            pl.semaphore_wait(ready, 1)

    def share(sums, which):
        for peer in (device(at_x(2), y, z, core), device(at_x(2), y, z, 1 - core), to["d"]):
            pltpu.make_async_remote_copy(
                src_ref=sums.at[orb], dst_ref=sums.at[orb], send_sem=shared.at[2 * which], recv_sem=shared.at[2 * which + 1],
                device_id=peer, device_id_type=MESH,
            ).start()

    def shared_by_all(sums, which):
        for end in range(2):
            three = sums.at[pl.ds(0, 3)]
            pltpu.make_async_copy(three, three, shared.at[2 * which + end]).wait()

    for step in plan()[0]:
        if step[0] == "send":
            copy(step[1]).start()
        elif step[0] == "product":
            product(step[1])
        elif step[0] == "share":
            share(dens, 0)
        elif step[0] == "weights":
            for table in tables:
                table.wait()
            weights()
        elif step[1] in loads:
            loads[step[1]].wait()
        elif step[1] == ("z",):
            neighbours()
        else:
            landed(step[1])

    share(tails, 1)
    shared_by_all(dens, 0)
    density[...] = dens[0] + dens[1] + dens[2] + dens[3]
    for key in todo:
        copy(key).wait_send()
    shared_by_all(tails, 1)
    last = tails[0] + tails[1] + tails[2] + tails[3]
    for half in range(2):
        density[1:2, pl.ds(half * 512 + TAIL, 512 - TAIL)] = last[half : half + 1]


def write_out(held, held_density, rotated, density, sem):
    copies = [pltpu.make_async_copy(held.at[g, m], rotated.at[g, m], sem.at[g * 4 + m]) for g in range(2) for m in range(4)]
    copies.append(pltpu.make_async_copy(held_density, density, sem.at[8]))
    for one in copies:
        one.start()
    for one in copies:
        one.wait()


def local(orbitals, slot_ids, slot_count, band_tiles, pattern, occupation):
    hbm, anywhere = (pl.BlockSpec(memory_space=s) for s in (pltpu.HBM, pl.ANY))
    n = len({v[3] for v in messages().values()})
    values, sums = ((2, 4, 2, 512, 128), jnp.bfloat16), ((2, 1024), jnp.float32)
    held = pl.pallas_call(
        kernel,
        out_shape=(pltpu.VMEM(*values), pltpu.VMEM(*sums)),
        in_specs=[hbm] * 6,
        scratch_shapes=[
            pltpu.SMEM((2, 4), jnp.int32),
            pltpu.SMEM((2,), jnp.int32),
            pltpu.SMEM((3, 16), jnp.int32),
            pltpu.VMEM((16, 128), jnp.float32),
            pltpu.VMEM((NZ, NY, 2, TILES, 8, 128), jnp.bfloat16),
            pltpu.VMEM((4, 2, 4, 2, 512, 128), jnp.bfloat16),
            pltpu.VMEM((2, 2, 4, 512, 128), jnp.bfloat16),
            pltpu.VMEM((4, 1536, 256), jnp.bfloat16),
            pltpu.VMEM((2, 512 - TAIL, 128), jnp.float32),
            pltpu.VMEM((4, 2, 1024), jnp.float32),
            pltpu.VMEM((4, 2, 512 - TAIL), jnp.float32),
            pltpu.SemaphoreType.DMA((n,)),
            pltpu.SemaphoreType.DMA((1,)),
            pltpu.SemaphoreType.DMA((4,)),
            pltpu.SemaphoreType.DMA((4,)),
            pltpu.SemaphoreType.REGULAR,
        ],
        compiler_params=pltpu.CompilerParams(collective_id=0, has_side_effects=True, vmem_limit_bytes=VMEM_BYTES),
    )(slot_ids, slot_count, pattern.T, band_tiles.reshape(48, 8, 128), orbitals.reshape(2, 4, 2, 512, 128), occupation)
    rotated, density = pl.pallas_call(
        write_out,
        out_shape=(jax.ShapeDtypeStruct(*values), jax.ShapeDtypeStruct(*sums)),
        in_specs=[anywhere] * 2,
        out_specs=(hbm, hbm),
        scratch_shapes=[pltpu.SemaphoreType.DMA((9,))],
        compiler_params=pltpu.CompilerParams(vmem_limit_bytes=1024 * 1024),
    )(*held)
    return rotated.reshape(2, 4, 1024, 128), density


def solution(mesh):
    return jax.shard_map(
        local,
        mesh=mesh,
        in_specs=(
            P("dom", None, None, "orb"),
            P("dom", None),
            P("dom"),
            P(None, None, "dom", "orb"),
            P(),
            P(None, "orb"),
        ),
        out_specs=(P("dom", None, None, "orb"), P("dom", None)),
        check_vma=False,
    )
```

```python
import functools
import heapq

import jax
import jax.numpy as jnp
from jax import lax
from jax.experimental import pallas as pl
from jax.experimental.pallas import tpu as pltpu
from jax.sharding import PartitionSpec as P

MESH = pl.DeviceIdType.MESH
NX, NY, NZ = 4, 4, 8
TILES = 46
A_TILES = 19
VMEM_BYTES = 67043328 - 2097152 - 8192
B_SETS = {1: (0, 1, -2, 3), -1: (-1, 2, -3, 4)}
CHUNKS = [(0, 0, 256), (0, 256, 256), (1, 0, 128), (1, 128, 128), (1, 256, 128), (1, 384, 64), (1, 448, 32), (1, 480, 32)]
UNITS = [(0, 0, 256), (0, 256, 256), (1, 0, 256), (1, 256, 128), (1, 384, 64), (1, 448, 32), (1, 480, 32)]
TAIL = 384
DEPTH = 2


def messages():
    tile = 8 * 128 * 2
    a, b = A_TILES * tile, (TILES - A_TILES) * tile
    out = {}

    def add(key, link, size, needs, group=None):
        out[key] = (link, size, needs, group or key)

    add(("swap",), "xs", a + b, [("tiles",)])
    half_of = {1: 0, -1: 1}
    mine = [[("z",)], [("z",), ("swap",)]]
    for n in range(1, 4):
        for w in range(2):
            for s in (1, -1):
                add(("Bz", s, n, w), ("z", s), b, mine[w] if n == 1 else [("Bz", n - 1, w)], ("Bz", n, w))
    for s in (1, -1):
        add(("Bz", s, 4, half_of[s]), ("z", s), b, [("Bz", 3, half_of[s])], ("Bz4",))
    for w in range(2):
        for s in (1, -1):
            add(("Ay1", s, w), ("y", s), a, mine[w], ("Ay1", w))
    for s in (1, -1):
        add(("Ay2", s, half_of[s]), ("y", s), a, [("Ay1", half_of[s])], ("Ay2",))
    sides = [("Ay1", 0), ("Ay1", 1)]
    have_a = {0: mine[1], -1: sides, 1: sides, 2: [("Ay2",)]}
    for dy in (0, -1, 1, 2):
        for n in range(1, 5):
            for s in (1, -1):
                before = [("Az", dy, n - 1)] if dy or n == 4 else [("Az", dy, n - 1, w) for w in range(2)]
                if n == 4:
                    add(("Az", s, dy, 4, half_of[s]), ("z", s), a, before, ("Az4",))
                elif dy == 0 and n < 3:
                    for w in range(2):
                        add(("Az", s, dy, n, w), ("z", s), a, mine[w] if n == 1 else [("Az", dy, n - 1, w)], ("Az", dy, n, w))
                else:
                    add(("Az", s, dy, n), ("z", s), 2 * a, have_a[dy] if n == 1 else before, ("Az", dy, n))
    have_b = {0: mine[1], 4: [("Bz4",)]}
    for n in range(1, 4):
        have_b[-n] = have_b[n] = [("Bz", n, 0), ("Bz", n, 1)]
    for dz in (0, -1, 1, -2, 2, -3, 3, 4):
        for s in (1, -1):
            onward = dz in B_SETS[s]
            group = ("By1", s, dz) if onward else ("By1", s)
            if dz == 0:
                for w in range(2):
                    add(("By1", s, dz, w), ("y", s), b, mine[w], group)
            else:
                add(("By1", s, dz), ("y", s), 2 * b, have_b[dz], group)
            if onward:
                add(("By2", s, dz), ("y", s), 2 * b, [("By1", s, dz)], ("By2",))
    row = 4 * 128 * 2
    for i in range(4):
        for s in (1, -1):
            add(("X1", s, i), ("x", s), 256 * row, [("own", i // 2)], ("X1", i))
    add(("Od",), "d", 2048 * row, [("own", 0), ("own", 1)])
    for k, (g, first, rows) in enumerate(CHUNKS):
        for s in (1, -1):
            add(("X2", s, k), ("x", s), rows * row, [("X1", g * 2 + first // 256)], ("X2", k))
        add(("Xd", k), "d", 2 * rows * row, [("X2", k)])
    return out


def chunks_of(u):
    if u >= len(UNITS):
        return []
    g, first, rows = UNITS[u]
    return [k for k, (cg, ca, _) in enumerate(CHUNKS) if cg == g and first <= ca < first + rows]


def plan():
    todo = messages()
    rate = {"d": 690e3}
    left, after = {}, {}
    for key, (_, _, needs, group) in todo.items():
        left.setdefault(group, set()).add(key)
        for need in needs:
            after.setdefault(need, []).append(key)

    @functools.lru_cache(None)
    def path(key):
        link, size, _, group = todo[key]
        return size / rate.get(link, 46.9e3) + 1.9 + max([path(k) for k in after.get(group, [])], default=0)

    free, here, due, order, pending = {}, set(), [], [], dict(todo)
    now = 0.0

    def send_ready():
        ready = [k for k, v in pending.items() if all(need in here for need in v[2])]
        for key in sorted(ready, key=lambda k: -path(k) if k[0][0] in "AB" else 0):
            link, size, _, group = todo[key]
            busy = [t for t in free.get(link, []) if t > now]
            if link[0] in "yz" and len(busy) >= DEPTH:
                continue
            pending.pop(key)
            links = [("x", 1), ("x", -1)] if link == "xs" else [link]
            start = max([now] + [t for one in links for t in free.get(one, [])[-1:]])
            end = start + size / rate.get(link, 46.9e3)
            for one in links:
                free.setdefault(one, []).append(end)
            heapq.heappush(due, (end + (1.0 if link == "d" else 1.9), len(order), key))
            order.append(("send", key))

    for i, group in enumerate([("tiles",), ("own", 0), ("own", 1), ("z",)]):
        heapq.heappush(due, (0.5 if group == ("z",) else 0.01 * i, i - 50, group))
        left[group] = {group}
    tiles_left = {g for g in left if g[0] in ("tiles", "swap", "Bz", "Bz4", "Ay1", "Ay2", "Az", "Az4", "By1", "By2")}
    weights, done = False, 0
    while due or done < len(UNITS):
        if due and due[0][0] <= now:
            key = heapq.heappop(due)[2]
            group = todo[key][3] if key in todo else key
            left[group].discard(key)
            if not left[group]:
                order.append(("wait", group))
                here.add(group)
                tiles_left.discard(group)
            send_ready()
            continue
        ready = weights and done < len(UNITS) and ("Od",) in here
        if ready:
            ready = all((t, k) in here for t in ("X2", "Xd") for k in chunks_of(done)) and all(("X2", k) in here for k in chunks_of(done + 1))
        if not weights and not tiles_left:
            order.append(("weights",))
            weights = True
            now += 0.7
        elif ready:
            if UNITS[done][:2] == (1, TAIL):
                order.append(("share",))
            order.append(("product", done))
            now += 0.4 + 0.4 * UNITS[done][2] / 128
            done += 1
        else:
            now = due[0][0]
    assert not pending
    return order, now


def kernel(
    ids_in, count_in, pattern_in, band, orbitals, occ_in, rotated, density,
    ids, count, pattern, occ, T, X, F, W, D, dens, tails, recv, sent, local, shared, ready,
):
    dom, orb = lax.axis_index("dom"), lax.axis_index("orb")
    x_lo, z, y = lax.div(dom, 32), lax.rem(lax.div(dom, 4), 8), lax.rem(dom, 4)
    x_hi, core = lax.div(orb, 2), lax.rem(orb, 2)
    x = x_hi * 2 + x_lo

    def at_x(step):
        return lax.rem(x + step + NX, NX)

    def at_y(step):
        return lax.rem(y + step + NY, NY)

    def at_z(step):
        return lax.rem(z + step + NZ, NZ)

    def device(px, py, pz, pc):
        return (lax.rem(px, 2) * 32 + pz * 4 + py, lax.div(px, 2) * 2 + pc)

    far = lax.div(at_x(2), 2) * 2 + core
    to = {"xs": device(x + 1 - 2 * x_lo, y, z, core), "d": device(x, y, z, 1 - core)}
    for s in (1, -1):
        to["x", s] = device(at_x(s), y, z, core)
        to["y", s] = device(x, at_y(s), z, core)
        to["z", s] = device(x, y, at_z(s), core)

    A, B, BOTH, ALL = pl.ds(0, A_TILES), pl.ds(A_TILES, TILES - A_TILES), pl.ds(0, 2), slice(None)

    def low(w=None):
        return BOTH if w is None else pl.ds(x_lo + w - 2 * w * x_lo, 1)

    def side(s):
        return 0 if s > 0 else 1

    todo = messages()
    groups = list(dict.fromkeys(v[3] for v in todo.values()))
    number = {group: i for i, group in enumerate(groups)}

    def ends(key):
        kind = key[0]
        if kind == "swap":
            return (T.at[z, y, x_lo],) * 2
        if kind == "Bz":
            _, s, n, w = key
            return (T.at[at_z(-(n - 1) * s), y, low(w), B],) * 2
        if kind == "Ay1":
            return (T.at[z, y, low(key[2]), A],) * 2
        if kind == "Ay2":
            return (T.at[z, at_y(-key[1]), low(key[2]), A],) * 2
        if kind == "Az":
            s, dy, n = key[1:4]
            return (T.at[at_z(-(n - 1) * s), at_y(dy), low(*key[4:]), A],) * 2
        if kind == "By1":
            return (T.at[at_z(key[2]), y, low(*key[3:]), B],) * 2
        if kind == "By2":
            return (T.at[at_z(key[2]), at_y(-key[1]), BOTH, B],) * 2
        if kind == "X1":
            _, s, i = key
            rows = pl.ds(i % 2 * 256, 256)
            return X.at[orb, i // 2, ALL, side(s), rows], F.at[side(s), i // 2, ALL, rows]
        if kind == "X2":
            _, s, k = key
            g, first, rows = CHUNKS[k]
            source = lax.div(at_x(-s), 2) * 2 + core
            return F.at[side(s), g, ALL, pl.ds(first, rows)], X.at[source, g, ALL, side(s), pl.ds(first, rows)]
        if kind == "Xd":
            g, first, rows = CHUNKS[key[1]]
            return (X.at[far, g, ALL, ALL, pl.ds(first, rows)],) * 2
        return (X.at[orb],) * 2

    def copy(key):
        src, dst = ends(key)
        return pltpu.make_async_remote_copy(
            src_ref=src, dst_ref=dst, send_sem=sent.at[0], recv_sem=recv.at[number[todo[key][3]]],
            device_id=to[todo[key][0]], device_id_type=MESH,
        )

    def landed(group):
        kind = group[0]
        one, two = pl.ds(0, 1), pl.ds(0, 2)
        if kind == "Bz":
            where = T.at[two, y, one, B]
        elif kind == "Bz4":
            where = T.at[z, y, BOTH, B]
        elif kind == "Ay1":
            where = T.at[z, two, one, A]
        elif kind == "Ay2":
            where = T.at[z, y, BOTH, A]
        elif kind == "Az":
            where = T.at[two, y, BOTH if len(group) == 3 else one, A]
        elif kind == "Az4":
            where = T.at[z, ALL, BOTH, A]
        elif kind == "By1":
            where = T.at[z, y, BOTH, B] if len(group) == 3 else T.at[pl.ds(0, 4), y, BOTH, B]
        elif kind == "By2":
            where = T.at[ALL, y, BOTH, B]
        elif kind == "X1":
            where = F.at[ALL, group[1] // 2, ALL, pl.ds(group[1] % 2 * 256, 256)]
        elif kind == "X2":
            g, first, rows = CHUNKS[group[1]]
            where = X.at[far, g, ALL, ALL, pl.ds(first, rows)]
        else:
            where = ends(group)[1]
        pltpu.make_async_copy(where, where, recv.at[number[group]]).wait()

    loads = {("tiles",): pltpu.make_async_copy(band.at[pl.ds(1, TILES)], T.at[z, y, x_lo], local.at[0])}
    for g in range(2):
        loads["own", g] = pltpu.make_async_copy(orbitals.at[g], X.at[orb, g], local.at[1 + g])
    tables = [
        pltpu.make_async_copy(here, there, local.at[3])
        for here, there in ((ids_in, ids), (count_in, count), (pattern_in, pattern), (occ_in, occ))
    ]

    def weights():
        for g in range(2):
            for pair in range(2):
                for at in range(3):
                    l = pair + at
                    for half in range(2):
                        m = pair * 2 + half
                        columns = pl.ds(half * 128, 128)
                        if abs(l - m) > 1:
                            W[g * 2 + pair, pl.ds(at * 512, 512), columns] = jnp.zeros((512, 128), jnp.bfloat16)
                            continue
                        source, target = ids[g, l], ids[g, m]
                        column = target - source + 1
                        inside = (column >= 0) & (column < 3)
                        column = jnp.clip(column, 0, 2)
                        keep = inside & (pattern[column, source] == 1) & (max(l, m) < count[g])
                        t = jnp.clip(source * 3 + column - 1, 0, TILES - 1)
                        scale = jnp.where(keep, jnp.float32(1), jnp.float32(0))
                        for low in range(2):
                            rows = T[:, :, low, t].astype(jnp.float32).reshape(256, 128) * scale
                            W[g * 2 + pair, pl.ds(at * 512 + low * 256, 256), columns] = rows.astype(jnp.bfloat16)

    def lane_sums(total):
        high = total.astype(jnp.bfloat16)
        rest = total - high.astype(jnp.float32)
        middle = rest.astype(jnp.bfloat16)
        low = (rest - middle.astype(jnp.float32)).astype(jnp.bfloat16)
        return lax.dot_general(
            jnp.ones((8, 384), jnp.bfloat16), jnp.concatenate([high, middle, low], axis=1),
            (((1,), (1,)), ((), ())), preferred_element_type=jnp.float32,
        )

    def product(u):
        g, first, n = UNITS[u]
        rows = pl.ds(first, n)
        total = jnp.zeros((2 * n, 128), jnp.float32)
        for pair in range(2):
            values = jnp.concatenate(
                [
                    jnp.concatenate([X[q, g, pair + at, half, rows] for at in range(3) for q in range(4)], axis=1)
                    for half in range(2)
                ],
                axis=0,
            )
            out = jnp.dot(values, W[g * 2 + pair], preferred_element_type=jnp.float32).astype(jnp.bfloat16)
            for which in range(2):
                m = pair * 2 + which
                one = out[:, which * 128 : which * 128 + 128]
                for half in range(2):
                    rotated[g, m, half, rows] = one[half * n : half * n + n]
                wide = one.astype(jnp.float32)
                total = total + wide * wide * occ[pl.ds(ids[g, m], 1), :]
        tail = g == 1 and first >= TAIL
        if tail:
            for half in range(2):
                D[half, pl.ds(first - TAIL, n)] = total[half * n : half * n + n]
            if u < len(UNITS) - 1:
                return
            n = 512 - TAIL
            summed = lane_sums(D[...].reshape(2 * n, 128))
            for half in range(2):
                tails[orb, pl.ds(half, 1)] = summed[0:1, half * n : half * n + n]
            return
        summed = lane_sums(total)
        for half in range(2):
            dens[orb, pl.ds(g, 1), pl.ds(half * 512 + first, n)] = summed[0:1, half * n : half * n + n]

    for load in loads.values():
        load.start()
    for table in tables:
        table.start()

    barrier = pltpu.get_barrier_semaphore()
    for step in (1, -1, 2):
        pl.semaphore_signal(barrier, inc=1, device_id=device(at_x(step), y, z, 0), device_id_type=MESH)
    for step in (1, -1):
        pl.semaphore_signal(barrier, inc=1, device_id=device(x, at_y(step), z, 1), device_id_type=MESH)
        pl.semaphore_signal(barrier, inc=1, device_id=device(x, y, at_z(step), 1), device_id_type=MESH)

    @pl.when(core == 1)
    def _():
        pl.semaphore_signal(barrier, inc=1, device_id=device(x, y, z, 0), device_id_type=MESH)

    @pl.when(core == 0)
    def _():
        pl.semaphore_wait(barrier, 7)
        pl.semaphore_signal(ready, inc=1, device_id=device(x, y, z, 1), device_id_type=MESH)

    @pl.when(core == 1)
    def _():
        pl.semaphore_wait(ready, 1)

    def neighbours():
        @pl.when(core == 1)
        def _():
            pl.semaphore_wait(barrier, 8)
            pl.semaphore_signal(ready, inc=1, device_id=device(x, y, z, 0), device_id_type=MESH)

        @pl.when(core == 0)
        def _():
            pl.semaphore_wait(ready, 1)

    def share(sums, which):
        for peer in (device(at_x(2), y, z, core), device(at_x(2), y, z, 1 - core), to["d"]):
            pltpu.make_async_remote_copy(
                src_ref=sums.at[orb], dst_ref=sums.at[orb], send_sem=shared.at[2 * which], recv_sem=shared.at[2 * which + 1],
                device_id=peer, device_id_type=MESH,
            ).start()

    def shared_by_all(sums, which):
        for end in range(2):
            three = sums.at[pl.ds(0, 3)]
            pltpu.make_async_copy(three, three, shared.at[2 * which + end]).wait()

    for step in plan()[0]:
        if step[0] == "send":
            copy(step[1]).start()
        elif step[0] == "product":
            product(step[1])
        elif step[0] == "share":
            share(dens, 0)
        elif step[0] == "weights":
            for table in tables:
                table.wait()
            weights()
        elif step[1] in loads:
            loads[step[1]].wait()
        elif step[1] == ("z",):
            neighbours()
        else:
            landed(step[1])

    share(tails, 1)
    shared_by_all(dens, 0)
    density[...] = dens[0] + dens[1] + dens[2] + dens[3]
    for key in todo:
        copy(key).wait_send()
    shared_by_all(tails, 1)
    last = tails[0] + tails[1] + tails[2] + tails[3]
    for half in range(2):
        density[1:2, pl.ds(half * 512 + TAIL, 512 - TAIL)] = last[half : half + 1]


def write_out(held, held_density, rotated, density, sem):
    copies = [pltpu.make_async_copy(held.at[g, m], rotated.at[g, m], sem.at[g * 4 + m]) for g in range(2) for m in range(4)]
    copies.append(pltpu.make_async_copy(held_density, density, sem.at[8]))
    for one in copies:
        one.start()
    for one in copies:
        one.wait()


def local(orbitals, slot_ids, slot_count, band_tiles, pattern, occupation):
    hbm, anywhere = (pl.BlockSpec(memory_space=s) for s in (pltpu.HBM, pl.ANY))
    n = len({v[3] for v in messages().values()})
    values, sums = ((2, 4, 2, 512, 128), jnp.bfloat16), ((2, 1024), jnp.float32)
    held = pl.pallas_call(
        kernel,
        out_shape=(pltpu.VMEM(*values), pltpu.VMEM(*sums)),
        in_specs=[hbm] * 6,
        scratch_shapes=[
            pltpu.SMEM((2, 4), jnp.int32),
            pltpu.SMEM((2,), jnp.int32),
            pltpu.SMEM((3, 16), jnp.int32),
            pltpu.VMEM((16, 128), jnp.float32),
            pltpu.VMEM((NZ, NY, 2, TILES, 8, 128), jnp.bfloat16),
            pltpu.VMEM((4, 2, 4, 2, 512, 128), jnp.bfloat16),
            pltpu.VMEM((2, 2, 4, 512, 128), jnp.bfloat16),
            pltpu.VMEM((4, 1536, 256), jnp.bfloat16),
            pltpu.VMEM((2, 512 - TAIL, 128), jnp.float32),
            pltpu.VMEM((4, 2, 1024), jnp.float32),
            pltpu.VMEM((4, 2, 512 - TAIL), jnp.float32),
            pltpu.SemaphoreType.DMA((n,)),
            pltpu.SemaphoreType.DMA((1,)),
            pltpu.SemaphoreType.DMA((4,)),
            pltpu.SemaphoreType.DMA((4,)),
            pltpu.SemaphoreType.REGULAR,
        ],
        compiler_params=pltpu.CompilerParams(collective_id=0, has_side_effects=True, vmem_limit_bytes=VMEM_BYTES),
    )(slot_ids, slot_count, pattern.T, band_tiles.reshape(48, 8, 128), orbitals.reshape(2, 4, 2, 512, 128), occupation)
    rotated, density = pl.pallas_call(
        write_out,
        out_shape=(jax.ShapeDtypeStruct(*values), jax.ShapeDtypeStruct(*sums)),
        in_specs=[anywhere] * 2,
        out_specs=(hbm, hbm),
        scratch_shapes=[pltpu.SemaphoreType.DMA((9,))],
        compiler_params=pltpu.CompilerParams(vmem_limit_bytes=1024 * 1024),
    )(*held)
    return rotated.reshape(2, 4, 1024, 128), density


def solution(mesh):
    return jax.shard_map(
        local,
        mesh=mesh,
        in_specs=(
            P("dom", None, None, "orb"),
            P("dom", None),
            P("dom"),
            P(None, None, "dom", "orb"),
            P(),
            P(None, "orb"),
        ),
        out_specs=(P("dom", None, None, "orb"), P("dom", None)),
        check_vma=False,
    )
```

```python
import functools
import heapq

import jax
import jax.numpy as jnp
from jax import lax
from jax.experimental import pallas as pl
from jax.experimental.pallas import tpu as pltpu
from jax.sharding import PartitionSpec as P

MESH = pl.DeviceIdType.MESH
NX, NY, NZ = 4, 4, 8
TILES = 46
A_TILES = 19
VMEM_BYTES = 67043328 - 2097152 - 8192
B_SETS = {1: (0, 1, -2, 3), -1: (-1, 2, -3, 4)}
CHUNKS = [(0, 0, 256), (0, 256, 256), (1, 0, 128), (1, 128, 128), (1, 256, 128), (1, 384, 64), (1, 448, 48), (1, 496, 16)]
UNITS = [(0, 0, 256), (0, 256, 256), (1, 0, 256), (1, 256, 128), (1, 384, 64), (1, 448, 64)]
TAIL = 384
DIRECT = len(CHUNKS) - 1
DEPTH = 2


def messages():
    tile = 8 * 128 * 2
    a, b = A_TILES * tile, (TILES - A_TILES) * tile
    out = {}

    def add(key, link, size, needs, group=None):
        out[key] = (link, size, needs, group or key)

    add(("swap",), "xs", a + b, [("tiles",)])
    half_of = {1: 0, -1: 1}
    mine = [[("z",)], [("z",), ("swap",)]]
    for n in range(1, 4):
        for w in range(2):
            for s in (1, -1):
                add(("Bz", s, n, w), ("z", s), b, mine[w] if n == 1 else [("Bz", n - 1, w)], ("Bz", n, w))
    for s in (1, -1):
        add(("Bz", s, 4, half_of[s]), ("z", s), b, [("Bz", 3, half_of[s])], ("Bz4",))
    for w in range(2):
        for s in (1, -1):
            add(("Ay1", s, w), ("y", s), a, mine[w], ("Ay1", w))
    for s in (1, -1):
        add(("Ay2", s, half_of[s]), ("y", s), a, [("Ay1", half_of[s])], ("Ay2",))
    sides = [("Ay1", 0), ("Ay1", 1)]
    have_a = {0: mine[1], -1: sides, 1: sides, 2: [("Ay2",)]}
    for dy in (0, -1, 1, 2):
        for n in range(1, 5):
            for s in (1, -1):
                before = [("Az", dy, n - 1)] if dy or n == 4 else [("Az", dy, n - 1, w) for w in range(2)]
                if n == 4:
                    add(("Az", s, dy, 4, half_of[s]), ("z", s), a, before, ("Az4",))
                elif dy == 0 and n < 3:
                    for w in range(2):
                        add(("Az", s, dy, n, w), ("z", s), a, mine[w] if n == 1 else [("Az", dy, n - 1, w)], ("Az", dy, n, w))
                else:
                    add(("Az", s, dy, n), ("z", s), 2 * a, have_a[dy] if n == 1 else before, ("Az", dy, n))
    have_b = {0: mine[1], 4: [("Bz4",)]}
    for n in range(1, 4):
        have_b[-n] = have_b[n] = [("Bz", n, 0), ("Bz", n, 1)]
    for dz in (0, -1, 1, -2, 2, -3, 3, 4):
        for s in (1, -1):
            onward = dz in B_SETS[s]
            group = ("By1", s, dz) if onward else ("By1", s)
            if dz == 0:
                for w in range(2):
                    add(("By1", s, dz, w), ("y", s), b, mine[w], group)
            else:
                add(("By1", s, dz), ("y", s), 2 * b, have_b[dz], group)
            if onward:
                add(("By2", s, dz), ("y", s), 2 * b, [("By1", s, dz)], ("By2",))
    row = 4 * 128 * 2
    for i in range(4):
        for s in (1, -1):
            add(("X1", s, i), ("x", s), 256 * row, [("own", i // 2)], ("X1", i))
    add(("Od",), "d", 2048 * row, [("own", 0), ("own", 1)])
    for k, (g, first, rows) in enumerate(CHUNKS):
        for s in (1, -1):
            add(("X2", s, k), ("x", s), rows * row, [("X1", g * 2 + first // 256)], ("X2", k))
            if k == DIRECT:
                add(("X2c", s, k), ("x", s), rows * row, [("X1", g * 2 + first // 256)], ("X2", k))
        if k < DIRECT:
            add(("Xd", k), "d", 2 * rows * row, [("X2", k)])
    return out


def chunks_of(u):
    if u >= len(UNITS):
        return []
    g, first, rows = UNITS[u]
    return [k for k, (cg, ca, _) in enumerate(CHUNKS) if cg == g and first <= ca < first + rows]


def plan():
    todo = messages()
    rate = {"d": 690e3}
    left, after = {}, {}
    for key, (_, _, needs, group) in todo.items():
        left.setdefault(group, set()).add(key)
        for need in needs:
            after.setdefault(need, []).append(key)

    @functools.lru_cache(None)
    def path(key):
        link, size, _, group = todo[key]
        return size / rate.get(link, 46.9e3) + 1.9 + max([path(k) for k in after.get(group, [])], default=0)

    free, here, due, order, pending = {}, set(), [], [], dict(todo)
    now = 0.0

    def send_ready():
        ready = [k for k, v in pending.items() if all(need in here for need in v[2])]
        for key in sorted(ready, key=lambda k: -path(k) if k[0][0] in "AB" else 0):
            link, size, _, group = todo[key]
            busy = [t for t in free.get(link, []) if t > now]
            if link[0] in "yz" and len(busy) >= DEPTH:
                continue
            pending.pop(key)
            links = [("x", 1), ("x", -1)] if link == "xs" else [link]
            start = max([now] + [t for one in links for t in free.get(one, [])[-1:]])
            end = start + size / rate.get(link, 46.9e3)
            for one in links:
                free.setdefault(one, []).append(end)
            heapq.heappush(due, (end + (1.0 if link == "d" else 1.9), len(order), key))
            order.append(("send", key))

    for i, group in enumerate([("tiles",), ("own", 0), ("own", 1), ("z",)]):
        heapq.heappush(due, (0.5 if group == ("z",) else 0.01 * i, i - 50, group))
        left[group] = {group}
    tiles_left = {g for g in left if g[0] in ("tiles", "swap", "Bz", "Bz4", "Ay1", "Ay2", "Az", "Az4", "By1", "By2")}
    weights, done = False, 0
    while due or done < len(UNITS):
        if due and due[0][0] <= now:
            key = heapq.heappop(due)[2]
            group = todo[key][3] if key in todo else key
            left[group].discard(key)
            if not left[group]:
                order.append(("wait", group))
                here.add(group)
                tiles_left.discard(group)
            send_ready()
            continue
        ready = weights and done < len(UNITS) and ("Od",) in here
        if ready:
            ready = all((t, k) in here for t in ("X2", "Xd") for k in chunks_of(done) if (t, k) in left)
            ready = ready and all(("X2", k) in here for k in chunks_of(done + 1) if k < DIRECT)
        if not weights and not tiles_left and ("X2", 2) in here:
            order.append(("weights",))
            weights = True
            now += 0.7
        elif ready:
            if UNITS[done][:2] == (1, TAIL):
                order.append(("share",))
            order.append(("product", done))
            now += 0.4 + 0.4 * UNITS[done][2] / 128
            done += 1
        else:
            now = due[0][0]
    assert not pending
    late = [("wait", group) for group in left if group[0] in ("Od", "Xd")]
    out = []
    for step in order:
        if step[0] == "product":
            out += [("wait", ("Od",))] * (step[1] == 0) + [("begin", step[1])] * (step[1] == len(UNITS) - 1)
            out += [("wait", ("Xd", k)) for k in chunks_of(step[1]) if k < DIRECT]
        if step not in late:
            out.append(step)
    return out, now


def kernel(
    ids_in, count_in, pattern_in, band, orbitals, occ_in, rotated, density,
    ids, count, pattern, occ, T, X, F, W, D, E, dens, tails, recv, sent, local, shared, ready,
):
    dom, orb = lax.axis_index("dom"), lax.axis_index("orb")
    x_lo, z, y = lax.div(dom, 32), lax.rem(lax.div(dom, 4), 8), lax.rem(dom, 4)
    x_hi, core = lax.div(orb, 2), lax.rem(orb, 2)
    x = x_hi * 2 + x_lo

    def at_x(step):
        return lax.rem(x + step + NX, NX)

    def at_y(step):
        return lax.rem(y + step + NY, NY)

    def at_z(step):
        return lax.rem(z + step + NZ, NZ)

    def device(px, py, pz, pc):
        return (lax.rem(px, 2) * 32 + pz * 4 + py, lax.div(px, 2) * 2 + pc)

    far = lax.div(at_x(2), 2) * 2 + core
    to = {"xs": device(x + 1 - 2 * x_lo, y, z, core), "d": device(x, y, z, 1 - core)}
    for s in (1, -1):
        to["x", s] = device(at_x(s), y, z, core)
        to["y", s] = device(x, at_y(s), z, core)
        to["z", s] = device(x, y, at_z(s), core)

    A, B, BOTH, ALL = pl.ds(0, A_TILES), pl.ds(A_TILES, TILES - A_TILES), pl.ds(0, 2), slice(None)

    def low(w=None):
        return BOTH if w is None else pl.ds(x_lo + w - 2 * w * x_lo, 1)

    def side(s):
        return 0 if s > 0 else 1

    todo = messages()
    groups = list(dict.fromkeys(v[3] for v in todo.values()))
    number = {group: i for i, group in enumerate(groups)}

    def ends(key):
        kind = key[0]
        if kind == "swap":
            return (T.at[z, y, x_lo],) * 2
        if kind == "Bz":
            _, s, n, w = key
            return (T.at[at_z(-(n - 1) * s), y, low(w), B],) * 2
        if kind == "Ay1":
            return (T.at[z, y, low(key[2]), A],) * 2
        if kind == "Ay2":
            return (T.at[z, at_y(-key[1]), low(key[2]), A],) * 2
        if kind == "Az":
            s, dy, n = key[1:4]
            return (T.at[at_z(-(n - 1) * s), at_y(dy), low(*key[4:]), A],) * 2
        if kind == "By1":
            return (T.at[at_z(key[2]), y, low(*key[3:]), B],) * 2
        if kind == "By2":
            return (T.at[at_z(key[2]), at_y(-key[1]), BOTH, B],) * 2
        if kind == "X1":
            _, s, i = key
            rows = pl.ds(i % 2 * 256, 256)
            return X.at[orb, i // 2, ALL, side(s), rows], F.at[side(s), i // 2, ALL, rows]
        if kind in ("X2", "X2c"):
            _, s, k = key
            g, first, rows = CHUNKS[k]
            source = lax.div(at_x(-s), 2) * 2 + core
            return F.at[side(s), g, ALL, pl.ds(first, rows)], X.at[source, g, ALL, side(s), pl.ds(first, rows)]
        if kind == "Xd":
            g, first, rows = CHUNKS[key[1]]
            return (X.at[far, g, ALL, ALL, pl.ds(first, rows)],) * 2
        return (X.at[orb],) * 2

    def copy(key):
        src, dst = ends(key)
        return pltpu.make_async_remote_copy(
            src_ref=src, dst_ref=dst, send_sem=sent.at[0], recv_sem=recv.at[number[todo[key][3]]],
            device_id=device(at_x(key[1]), y, z, 1 - core) if key[0] == "X2c" else to[todo[key][0]], device_id_type=MESH,
        )

    def landed(group):
        kind = group[0]
        one, two = pl.ds(0, 1), pl.ds(0, 2)
        if kind == "Bz":
            where = T.at[two, y, one, B]
        elif kind == "Bz4":
            where = T.at[z, y, BOTH, B]
        elif kind == "Ay1":
            where = T.at[z, two, one, A]
        elif kind == "Ay2":
            where = T.at[z, y, BOTH, A]
        elif kind == "Az":
            where = T.at[two, y, BOTH if len(group) == 3 else one, A]
        elif kind == "Az4":
            where = T.at[z, ALL, BOTH, A]
        elif kind == "By1":
            where = T.at[z, y, BOTH, B] if len(group) == 3 else T.at[pl.ds(0, 4), y, BOTH, B]
        elif kind == "By2":
            where = T.at[ALL, y, BOTH, B]
        elif kind == "X1":
            where = F.at[ALL, group[1] // 2, ALL, pl.ds(group[1] % 2 * 256, 256)]
        elif kind == "X2":
            g, first, rows = CHUNKS[group[1]]
            orbs = pl.ds(lax.div(at_x(2), 2) * 2, 2) if group[1] == DIRECT else far
            where = X.at[orbs, g, ALL, ALL, pl.ds(first, rows)]
        else:
            where = ends(group)[1]
        pltpu.make_async_copy(where, where, recv.at[number[group]]).wait()

    loads = {("tiles",): pltpu.make_async_copy(band.at[pl.ds(1, TILES)], T.at[z, y, x_lo], local.at[0])}
    for g in range(2):
        loads["own", g] = pltpu.make_async_copy(orbitals.at[g], X.at[orb, g], local.at[1 + g])
    tables = [
        pltpu.make_async_copy(here, there, local.at[3])
        for here, there in ((ids_in, ids), (count_in, count), (pattern_in, pattern), (occ_in, occ))
    ]

    def weights():
        for g in range(2):
            for pair in range(2):
                for at in range(3):
                    l = pair + at
                    for half in range(2):
                        m = pair * 2 + half
                        columns = pl.ds(half * 128, 128)
                        if abs(l - m) > 1:
                            W[g * 2 + pair, pl.ds(at * 512, 512), columns] = jnp.zeros((512, 128), jnp.bfloat16)
                            continue
                        source, target = ids[g, l], ids[g, m]
                        column = target - source + 1
                        inside = (column >= 0) & (column < 3)
                        column = jnp.clip(column, 0, 2)
                        keep = inside & (pattern[column, source] == 1) & (max(l, m) < count[g])
                        t = jnp.clip(source * 3 + column - 1, 0, TILES - 1)
                        scale = jnp.where(keep, jnp.float32(1), jnp.float32(0))
                        for low in range(2):
                            rows = T[:, :, low, t].astype(jnp.float32).reshape(256, 128) * scale
                            W[g * 2 + pair, pl.ds(at * 512 + low * 256, 256), columns] = rows.astype(jnp.bfloat16)

    def lane_sums(total):
        high = total.astype(jnp.bfloat16)
        rest = total - high.astype(jnp.float32)
        middle = rest.astype(jnp.bfloat16)
        low = (rest - middle.astype(jnp.float32)).astype(jnp.bfloat16)
        return lax.dot_general(
            jnp.ones((8, 384), jnp.bfloat16), jnp.concatenate([high, middle, low], axis=1),
            (((1,), (1,)), ((), ())), preferred_element_type=jnp.float32,
        )

    def multiply(u, pair, orbs):
        g, first, n = UNITS[u]
        parts = [(at, q) for at in range(3) for q in orbs]
        values = jnp.concatenate(
            [jnp.concatenate([X[q, g, pair + at, half, pl.ds(first, n)] for at, q in parts], axis=1) for half in range(2)], axis=0
        )
        if len(orbs) == 4:
            tiles = W[g * 2 + pair]
        else:
            tiles = jnp.concatenate([W[g * 2 + pair, pl.ds(pl.multiple_of(at * 512 + q * 128, 128), 128)] for at, q in parts], axis=0)
        return jnp.dot(values, tiles, preferred_element_type=jnp.float32)

    def begin(u):
        for pair in range(2):
            E[pair] = multiply(u, pair, (orb, x_hi * 2 + 1 - core, far))

    def product(u):
        g, first, n = UNITS[u]
        rows = pl.ds(first, n)
        total = jnp.zeros((2 * n, 128), jnp.float32)
        for pair in range(2):
            if u < len(UNITS) - 1:
                out = multiply(u, pair, range(4))
            else:
                out = E[pair] + multiply(u, pair, (lax.div(at_x(2), 2) * 2 + 1 - core,))
            out = out.astype(jnp.bfloat16)
            for which in range(2):
                m = pair * 2 + which
                one = out[:, which * 128 : which * 128 + 128]
                for half in range(2):
                    rotated[g, m, half, rows] = one[half * n : half * n + n]
                wide = one.astype(jnp.float32)
                total = total + wide * wide * occ[pl.ds(ids[g, m], 1), :]
        tail = g == 1 and first >= TAIL
        if tail:
            for half in range(2):
                D[half, pl.ds(first - TAIL, n)] = total[half * n : half * n + n]
            if u < len(UNITS) - 1:
                return
            n = 512 - TAIL
            summed = lane_sums(D[...].reshape(2 * n, 128))
            for half in range(2):
                tails[orb, pl.ds(half, 1)] = summed[0:1, half * n : half * n + n]
            return
        summed = lane_sums(total)
        for half in range(2):
            dens[orb, pl.ds(g, 1), pl.ds(half * 512 + first, n)] = summed[0:1, half * n : half * n + n]

    barrier = pltpu.get_barrier_semaphore()
    for step in (1, -1):
        pl.semaphore_signal(barrier, inc=1, device_id=device(at_x(step), y, z, 0), device_id_type=MESH)
    for step in (1, -1):
        pl.semaphore_signal(barrier, inc=1, device_id=device(x, at_y(step), z, 1), device_id_type=MESH)
        pl.semaphore_signal(barrier, inc=1, device_id=device(x, y, at_z(step), 1), device_id_type=MESH)

    @pl.when(core == 1)
    def _():
        pl.semaphore_signal(barrier, inc=1, device_id=device(x, y, z, 0), device_id_type=MESH)

    for load in loads.values():
        load.start()
    for table in tables:
        table.start()

    @pl.when(core == 0)
    def _():
        pl.semaphore_wait(barrier, 5)
        pl.semaphore_signal(ready, inc=1, device_id=device(x, y, z, 1), device_id_type=MESH)

    @pl.when(core == 1)
    def _():
        pl.semaphore_wait(ready, 1)

    def neighbours():
        @pl.when(core == 1)
        def _():
            pl.semaphore_wait(barrier, 8)
            pl.semaphore_signal(ready, inc=1, device_id=device(x, y, z, 0), device_id_type=MESH)

        @pl.when(core == 0)
        def _():
            pl.semaphore_wait(ready, 1)

    def share(sums, which):
        for peer in (device(at_x(2), y, z, core), device(at_x(2), y, z, 1 - core), to["d"]):
            pltpu.make_async_remote_copy(
                src_ref=sums.at[orb], dst_ref=sums.at[orb], send_sem=shared.at[2 * which], recv_sem=shared.at[2 * which + 1],
                device_id=peer, device_id_type=MESH,
            ).start()

    def shared_by_all(sums, which):
        for end in range(2):
            three = sums.at[pl.ds(0, 3)]
            pltpu.make_async_copy(three, three, shared.at[2 * which + end]).wait()

    for step in plan()[0]:
        if step[0] == "send":
            copy(step[1]).start()
        elif step[0] == "product":
            product(step[1])
        elif step[0] == "begin":
            begin(step[1])
        elif step[0] == "share":
            share(dens, 0)
        elif step[0] == "weights":
            for table in tables:
                table.wait()
            weights()
        elif step[1] in loads:
            loads[step[1]].wait()
        elif step[1] == ("z",):
            neighbours()
        else:
            landed(step[1])

    share(tails, 1)
    shared_by_all(dens, 0)
    density[...] = dens[0] + dens[1] + dens[2] + dens[3]
    for key in todo:
        copy(key).wait_send()
    shared_by_all(tails, 1)
    last = tails[0] + tails[1] + tails[2] + tails[3]
    for half in range(2):
        density[1:2, pl.ds(half * 512 + TAIL, 512 - TAIL)] = last[half : half + 1]


def write_out(held, held_density, rotated, density, sem):
    copies = [pltpu.make_async_copy(held.at[g, m], rotated.at[g, m], sem.at[g * 4 + m]) for g in range(2) for m in range(4)]
    copies.append(pltpu.make_async_copy(held_density, density, sem.at[8]))
    for one in copies:
        one.start()
    for one in copies:
        one.wait()


def local(orbitals, slot_ids, slot_count, band_tiles, pattern, occupation):
    hbm, anywhere = (pl.BlockSpec(memory_space=s) for s in (pltpu.HBM, pl.ANY))
    n = len({v[3] for v in messages().values()})
    values, sums = ((2, 4, 2, 512, 128), jnp.bfloat16), ((2, 1024), jnp.float32)
    held = pl.pallas_call(
        kernel,
        out_shape=(pltpu.VMEM(*values), pltpu.VMEM(*sums)),
        in_specs=[hbm] * 6,
        scratch_shapes=[
            pltpu.SMEM((2, 4), jnp.int32),
            pltpu.SMEM((2,), jnp.int32),
            pltpu.SMEM((3, 16), jnp.int32),
            pltpu.VMEM((16, 128), jnp.float32),
            pltpu.VMEM((NZ, NY, 2, TILES, 8, 128), jnp.bfloat16),
            pltpu.VMEM((4, 2, 4, 2, 512, 128), jnp.bfloat16),
            pltpu.VMEM((2, 2, 4, 512, 128), jnp.bfloat16),
            pltpu.VMEM((4, 1536, 256), jnp.bfloat16),
            pltpu.VMEM((2, 512 - TAIL, 128), jnp.float32),
            pltpu.VMEM((2, 2 * UNITS[-1][2], 256), jnp.float32),
            pltpu.VMEM((4, 2, 1024), jnp.float32),
            pltpu.VMEM((4, 2, 512 - TAIL), jnp.float32),
            pltpu.SemaphoreType.DMA((n,)),
            pltpu.SemaphoreType.DMA((1,)),
            pltpu.SemaphoreType.DMA((4,)),
            pltpu.SemaphoreType.DMA((4,)),
            pltpu.SemaphoreType.REGULAR,
        ],
        compiler_params=pltpu.CompilerParams(collective_id=0, has_side_effects=True, vmem_limit_bytes=VMEM_BYTES),
    )(slot_ids, slot_count, pattern.T, band_tiles.reshape(48, 8, 128), orbitals.reshape(2, 4, 2, 512, 128), occupation)
    rotated, density = pl.pallas_call(
        write_out,
        out_shape=(jax.ShapeDtypeStruct(*values), jax.ShapeDtypeStruct(*sums)),
        in_specs=[anywhere] * 2,
        out_specs=(hbm, hbm),
        scratch_shapes=[pltpu.SemaphoreType.DMA((9,))],
        compiler_params=pltpu.CompilerParams(vmem_limit_bytes=1024 * 1024),
    )(*held)
    return rotated.reshape(2, 4, 1024, 128), density


def solution(mesh):
    return jax.shard_map(
        local,
        mesh=mesh,
        in_specs=(
            P("dom", None, None, "orb"),
            P("dom", None),
            P("dom"),
            P(None, None, "dom", "orb"),
            P(),
            P(None, "orb"),
        ),
        out_specs=(P("dom", None, None, "orb"), P("dom", None)),
        check_vma=False,
    )
```

```python
import functools
import heapq

import jax
import jax.numpy as jnp
from jax import lax
from jax.experimental import pallas as pl
from jax.experimental.pallas import tpu as pltpu
from jax.sharding import PartitionSpec as P

MESH = pl.DeviceIdType.MESH
NX, NY, NZ = 4, 4, 8
TILES = 46
A_TILES = 18
VMEM_BYTES = 67043328 - 2097152 - 8192
B_SETS = {1: (0, 1, -2, 3), -1: (-1, 2, -3, 4)}
CHUNKS = [(0, 0, 256), (0, 256, 256), (1, 0, 128), (1, 128, 128), (1, 256, 128), (1, 384, 64), (1, 448, 48), (1, 496, 16)]
UNITS = [(0, 0, 256), (0, 256, 256), (1, 0, 256), (1, 256, 128), (1, 384, 64), (1, 448, 64)]
TAIL = 384
SHARED = 4
DIRECT = len(CHUNKS) - 1
DEPTH = 3


def messages():
    tile = 8 * 128 * 2
    a, b = A_TILES * tile, (TILES - A_TILES) * tile
    out = {}

    def add(key, link, size, needs, group=None):
        out[key] = (link, size, needs, group or key)

    add(("swap",), "xs", a + b, [("tiles",)])
    half_of = {1: 0, -1: 1}
    mine = [[("z",)], [("z",), ("swap",)]]
    for n in range(1, 4):
        for w in range(2):
            for s in (1, -1):
                add(("Bz", s, n, w), ("z", s), b, mine[w] if n == 1 else [("Bz", n - 1, w)], ("Bz", n, w))
    for s in (1, -1):
        add(("Bz", s, 4, half_of[s]), ("z", s), b, [("Bz", 3, half_of[s])], ("Bz4",))
    for w in range(2):
        for s in (1, -1):
            add(("Ay1", s, w), ("y", s), a, mine[w], ("Ay1", w))
    for s in (1, -1):
        add(("Ay2", s, half_of[s]), ("y", s), a, [("Ay1", half_of[s])], ("Ay2",))
    sides = [("Ay1", 0), ("Ay1", 1)]
    have_a = {0: mine[1], -1: sides, 1: sides, 2: [("Ay2",)]}
    for dy in (0, -1, 1, 2):
        for n in range(1, 5):
            for s in (1, -1):
                before = [("Az", dy, n - 1)] if dy or n == 4 else [("Az", dy, n - 1, w) for w in range(2)]
                if n == 4:
                    add(("Az", s, dy, 4, half_of[s]), ("z", s), a, before, ("Az4",))
                elif dy == 0 and n < 3:
                    for w in range(2):
                        add(("Az", s, dy, n, w), ("z", s), a, mine[w] if n == 1 else [("Az", dy, n - 1, w)], ("Az", dy, n, w))
                else:
                    add(("Az", s, dy, n), ("z", s), 2 * a, have_a[dy] if n == 1 else before, ("Az", dy, n))
    have_b = {0: mine[1], 4: [("Bz4",)]}
    for n in range(1, 4):
        have_b[-n] = have_b[n] = [("Bz", n, 0), ("Bz", n, 1)]
    for dz in (0, -1, 1, -2, 2, -3, 3, 4):
        for s in (1, -1):
            onward = dz in B_SETS[s]
            group = ("By1", s, dz) if onward else ("By1", s)
            if dz == 0:
                for w in range(2):
                    add(("By1", s, dz, w), ("y", s), b, mine[w], group)
            else:
                add(("By1", s, dz), ("y", s), 2 * b, have_b[dz], group)
            if onward:
                add(("By2", s, dz), ("y", s), 2 * b, [("By1", s, dz)], ("By2",))
    row = 4 * 128 * 2
    for i in range(4):
        for s in (1, -1):
            add(("X1", s, i), ("x", s), 256 * row, [("own", i // 2)], ("X1", i))
    add(("Od",), "d", 2048 * row, [("own", 0), ("own", 1), ("z",)])
    for k, (g, first, rows) in enumerate(CHUNKS):
        for s in (1, -1):
            add(("X2", s, k), ("x", s), rows * row, [("X1", g * 2 + first // 256)], ("X2", k))
            if k == DIRECT:
                add(("X2c", s, k), ("x", s), rows * row, [("X1", g * 2 + first // 256)], ("X2", k))
        if k < DIRECT:
            add(("Xd", k), "d", 2 * rows * row, [("X2", k)])
    return out


def chunks_of(u):
    if u >= len(UNITS):
        return []
    g, first, rows = UNITS[u]
    return [k for k, (cg, ca, _) in enumerate(CHUNKS) if cg == g and first <= ca < first + rows]


def plan():
    todo = messages()
    rate = {"d": 690e3}
    left, after = {}, {}
    for key, (_, _, needs, group) in todo.items():
        left.setdefault(group, set()).add(key)
        for need in needs:
            after.setdefault(need, []).append(key)

    @functools.lru_cache(None)
    def path(key):
        link, size, _, group = todo[key]
        return size / rate.get(link, 46.9e3) + 1.9 + max([path(k) for k in after.get(group, [])], default=0)

    free, here, due, order, pending = {}, set(), [], [], dict(todo)
    now = 0.0

    def send_ready():
        ready = [k for k, v in pending.items() if all(need in here for need in v[2])]
        for key in sorted(ready, key=lambda k: -path(k) if k[0][0] in "AB" else 0):
            link, size, _, group = todo[key]
            busy = [t for t in free.get(link, []) if t > now]
            if link[0] in "yz" and len(busy) >= DEPTH:
                continue
            pending.pop(key)
            links = [("x", 1), ("x", -1)] if link == "xs" else [link]
            start = max([now] + [t for one in links for t in free.get(one, [])[-1:]])
            end = start + size / rate.get(link, 46.9e3)
            for one in links:
                free.setdefault(one, []).append(end)
            heapq.heappush(due, (end + (1.0 if link == "d" else 1.9), len(order), key))
            order.append(("send", key))

    for i, group in enumerate([("tiles",), ("own", 0), ("own", 1), ("z",)]):
        heapq.heappush(due, (0.5 if group == ("z",) else 0.01 * i, i - 50, group))
        left[group] = {group}
    first = {g for g in left if g[0] not in ("X2", "Xd", "Od")} | {("X2", 0)}
    while not first <= here:
        now = max(now, due[0][0])
        key = heapq.heappop(due)[2]
        group = todo[key][3] if key in todo else key
        left[group].discard(key)
        if left[group] or group not in first:
            continue
        order.append(("wait", group))
        here.add(group)
        send_ready()

    def forward(*chunks):
        return [step for k in chunks for step in [("wait", ("X2", k))] + [("send", ("Xd", k))] * (k < DIRECT)]

    def product(u):
        return [("wait", ("Xd", k)) for k in chunks_of(u) if k < DIRECT] + [("product", u)]

    order += forward(1) + [("weights",), ("wait", ("Od",))] + forward(2) + product(0) + forward(3) + product(1)
    order += forward(4) + product(2) + forward(5) + product(3) + forward(6) + product(4) + [("share",)] + forward(DIRECT) + [("begin", 5)] + product(5)
    return order


def kernel(
    ids_in, count_in, pattern_in, band, orbitals, occ_in, rotated, density,
    ids, count, pattern, occ, T, X, F, W, D, E, dens, tails, recv, sent, local, shared, ready,
):
    dom, orb = lax.axis_index("dom"), lax.axis_index("orb")
    x_lo, z, y = lax.div(dom, 32), lax.rem(lax.div(dom, 4), 8), lax.rem(dom, 4)
    x_hi, core = lax.div(orb, 2), lax.rem(orb, 2)
    x = x_hi * 2 + x_lo

    def at_x(step):
        return lax.rem(x + step + NX, NX)

    def at_y(step):
        return lax.rem(y + step + NY, NY)

    def at_z(step):
        return lax.rem(z + step + NZ, NZ)

    def device(px, py, pz, pc):
        return (lax.rem(px, 2) * 32 + pz * 4 + py, lax.div(px, 2) * 2 + pc)

    far = lax.div(at_x(2), 2) * 2 + core
    to = {"xs": device(x + 1 - 2 * x_lo, y, z, core), "d": device(x, y, z, 1 - core)}
    for s in (1, -1):
        to["x", s] = device(at_x(s), y, z, core)
        to["y", s] = device(x, at_y(s), z, core)
        to["z", s] = device(x, y, at_z(s), core)

    A, B, BOTH, ALL = pl.ds(0, A_TILES), pl.ds(A_TILES, TILES - A_TILES), pl.ds(0, 2), slice(None)

    def low(w=None):
        return BOTH if w is None else pl.ds(x_lo + w - 2 * w * x_lo, 1)

    def side(s):
        return 0 if s > 0 else 1

    todo = messages()
    groups = list(dict.fromkeys(v[3] for v in todo.values()))
    number = {group: i for i, group in enumerate(groups)}

    def ends(key):
        kind = key[0]
        if kind == "swap":
            return (T.at[z, y, x_lo],) * 2
        if kind == "Bz":
            _, s, n, w = key
            return (T.at[at_z(-(n - 1) * s), y, low(w), B],) * 2
        if kind == "Ay1":
            return (T.at[z, y, low(key[2]), A],) * 2
        if kind == "Ay2":
            return (T.at[z, at_y(-key[1]), low(key[2]), A],) * 2
        if kind == "Az":
            s, dy, n = key[1:4]
            return (T.at[at_z(-(n - 1) * s), at_y(dy), low(*key[4:]), A],) * 2
        if kind == "By1":
            return (T.at[at_z(key[2]), y, low(*key[3:]), B],) * 2
        if kind == "By2":
            return (T.at[at_z(key[2]), at_y(-key[1]), BOTH, B],) * 2
        if kind == "X1":
            _, s, i = key
            rows = pl.ds(i % 2 * 256, 256)
            return X.at[orb, i // 2, ALL, side(s), rows], F.at[side(s), i // 2, ALL, rows]
        if kind in ("X2", "X2c"):
            _, s, k = key
            g, first, rows = CHUNKS[k]
            source = lax.div(at_x(-s), 2) * 2 + core
            return F.at[side(s), g, ALL, pl.ds(first, rows)], X.at[source, g, ALL, side(s), pl.ds(first, rows)]
        if kind == "Xd":
            g, first, rows = CHUNKS[key[1]]
            return (X.at[far, g, ALL, ALL, pl.ds(first, rows)],) * 2
        return (X.at[orb],) * 2

    def copy(key):
        src, dst = ends(key)
        return pltpu.make_async_remote_copy(
            src_ref=src, dst_ref=dst, send_sem=sent.at[0], recv_sem=recv.at[number[todo[key][3]]],
            device_id=device(at_x(key[1]), y, z, 1 - core) if key[0] == "X2c" else to[todo[key][0]], device_id_type=MESH,
        )

    def landed(group):
        kind = group[0]
        one, two = pl.ds(0, 1), pl.ds(0, 2)
        if kind == "Bz":
            where = T.at[two, y, one, B]
        elif kind == "Bz4":
            where = T.at[z, y, BOTH, B]
        elif kind == "Ay1":
            where = T.at[z, two, one, A]
        elif kind == "Ay2":
            where = T.at[z, y, BOTH, A]
        elif kind == "Az":
            where = T.at[two, y, BOTH if len(group) == 3 else one, A]
        elif kind == "Az4":
            where = T.at[z, ALL, BOTH, A]
        elif kind == "By1":
            where = T.at[z, y, BOTH, B] if len(group) == 3 else T.at[pl.ds(0, 4), y, BOTH, B]
        elif kind == "By2":
            where = T.at[ALL, y, BOTH, B]
        elif kind == "X1":
            where = F.at[ALL, group[1] // 2, ALL, pl.ds(group[1] % 2 * 256, 256)]
        elif kind == "X2":
            g, first, rows = CHUNKS[group[1]]
            orbs = pl.ds(lax.div(at_x(2), 2) * 2, 2) if group[1] == DIRECT else far
            where = X.at[orbs, g, ALL, ALL, pl.ds(first, rows)]
        else:
            where = ends(group)[1]
        pltpu.make_async_copy(where, where, recv.at[number[group]]).wait()

    loads = {("tiles",): pltpu.make_async_copy(band.at[pl.ds(1, TILES)], T.at[z, y, x_lo], local.at[0])}
    for g in range(2):
        loads["own", g] = pltpu.make_async_copy(orbitals.at[g], X.at[orb, g], local.at[1 + g])
    tables = [
        pltpu.make_async_copy(here, there, local.at[3])
        for here, there in ((ids_in, ids), (count_in, count), (pattern_in, pattern), (occ_in, occ))
    ]

    def weights():
        for g in range(2):
            for pair in range(2):
                for at in range(3):
                    l = pair + at
                    for half in range(2):
                        m = pair * 2 + half
                        columns = pl.ds(half * 128, 128)
                        if abs(l - m) > 1:
                            W[g * 2 + pair, pl.ds(at * 512, 512), columns] = jnp.zeros((512, 128), jnp.bfloat16)
                            continue
                        source, target = ids[g, l], ids[g, m]
                        column = target - source + 1
                        inside = (column >= 0) & (column < 3)
                        column = jnp.clip(column, 0, 2)
                        keep = inside & (pattern[column, source] == 1) & (max(l, m) < count[g])
                        t = jnp.clip(source * 3 + column - 1, 0, TILES - 1)
                        scale = jnp.where(keep, jnp.float32(1), jnp.float32(0))
                        for low in range(2):
                            rows = T[:, :, low, t].astype(jnp.float32).reshape(256, 128) * scale
                            W[g * 2 + pair, pl.ds(at * 512 + low * 256, 256), columns] = rows.astype(jnp.bfloat16)

    def lane_sums(u):
        g, first, n = UNITS[u]
        for half in range(2):
            total = D[g, half, pl.ds(first, n)]
            dens[orb, pl.ds(g, 1), pl.ds(half * 512 + first, n)] = jnp.sum(total.T, axis=0, keepdims=True)

    def multiply(u, pair, orbs):
        g, first, n = UNITS[u]
        parts = [(at, q) for at in range(3) for q in orbs]
        values = jnp.concatenate(
            [jnp.concatenate([X[q, g, pair + at, half, pl.ds(first, n)] for at, q in parts], axis=1) for half in range(2)], axis=0
        )
        if len(orbs) == 4:
            tiles = W[g * 2 + pair]
        else:
            tiles = jnp.concatenate([W[g * 2 + pair, pl.ds(pl.multiple_of(at * 512 + q * 128, 128), 128)] for at, q in parts], axis=0)
        return jnp.dot(values, tiles, preferred_element_type=jnp.float32)

    def begin(u):
        for pair in range(2):
            E[pair] = multiply(u, pair, (orb, x_hi * 2 + 1 - core, far))

    def product(u):
        g, first, n = UNITS[u]
        rows = pl.ds(first, n)
        total = jnp.zeros((2 * n, 128), jnp.float32)
        for pair in range(2):
            if u < len(UNITS) - 1:
                out = multiply(u, pair, range(4))
            else:
                out = E[pair] + multiply(u, pair, (lax.div(at_x(2), 2) * 2 + 1 - core,))
            out = out.astype(jnp.bfloat16)
            for which in range(2):
                m = pair * 2 + which
                one = out[:, which * 128 : which * 128 + 128]
                for half in range(2):
                    rotated[g, m, half, rows] = one[half * n : half * n + n]
                wide = one.astype(jnp.float32)
                total = total + wide * wide * occ[pl.ds(ids[g, m], 1), :]
        for half in range(2):
            D[g, half, rows] = total[half * n : half * n + n]
        if 1 <= u <= SHARED:
            lane_sums(u - 1)
        if u == len(UNITS) - 1:
            for half in range(2):
                tails[orb, pl.ds(half, 1)] = jnp.sum(D[1, half, pl.ds(TAIL, 512 - TAIL)].T, axis=0, keepdims=True)

    barrier = pltpu.get_barrier_semaphore()
    for step in (1, -1):
        pl.semaphore_signal(barrier, inc=1, device_id=to["x", step], device_id_type=MESH)
    for step in (1, -1):
        pl.semaphore_signal(barrier, inc=1, device_id=device(x, at_y(step), z, 0), device_id_type=MESH)
        pl.semaphore_signal(barrier, inc=1, device_id=device(x, y, at_z(step), 0), device_id_type=MESH)

    @pl.when(core == 1)
    def _():
        pl.semaphore_signal(barrier, inc=1, device_id=device(x, y, z, 0), device_id_type=MESH)

    for load in loads.values():
        load.start()
    for table in tables:
        table.start()

    @pl.when(core == 0)
    def _():
        pl.semaphore_wait(barrier, 11)
        pl.semaphore_signal(ready, inc=1, device_id=device(x, y, z, 1), device_id_type=MESH)

    @pl.when(core == 1)
    def _():
        pl.semaphore_wait(barrier, 2)

    def neighbours():
        @pl.when(core == 1)
        def _():
            pl.semaphore_wait(ready, 1)

    def share(sums, which):
        for peer in (device(at_x(2), y, z, core), device(at_x(2), y, z, 1 - core), to["d"]):
            pltpu.make_async_remote_copy(
                src_ref=sums.at[orb], dst_ref=sums.at[orb], send_sem=shared.at[2 * which], recv_sem=shared.at[2 * which + 1],
                device_id=peer, device_id_type=MESH,
            ).start()

    def shared_by_all(sums, which):
        for end in range(2):
            three = sums.at[pl.ds(0, 3)]
            pltpu.make_async_copy(three, three, shared.at[2 * which + end]).wait()

    for step in plan():
        if step[0] == "send":
            copy(step[1]).start()
        elif step[0] == "product":
            product(step[1])
        elif step[0] == "begin":
            begin(step[1])
        elif step[0] == "share":
            share(dens, 0)
        elif step[0] == "weights":
            for table in tables:
                table.wait()
            weights()
        elif step[1] in loads:
            loads[step[1]].wait()
        elif step[1] == ("z",):
            neighbours()
        else:
            landed(step[1])

    share(tails, 1)
    shared_by_all(dens, 0)
    density[...] = dens[0] + dens[1] + dens[2] + dens[3]
    for key in todo:
        copy(key).wait_send()
    shared_by_all(tails, 1)
    last = tails[0] + tails[1] + tails[2] + tails[3]
    for half in range(2):
        density[1:2, pl.ds(half * 512 + TAIL, 512 - TAIL)] = last[half : half + 1]


def write_out(held, held_density, rotated, density, sem):
    copies = [pltpu.make_async_copy(held.at[g, m], rotated.at[g, m], sem.at[g * 4 + m]) for g in range(2) for m in range(4)]
    copies.append(pltpu.make_async_copy(held_density, density, sem.at[8]))
    for one in copies:
        one.start()
    for one in copies:
        one.wait()


def local(orbitals, slot_ids, slot_count, band_tiles, pattern, occupation):
    hbm, anywhere = (pl.BlockSpec(memory_space=s) for s in (pltpu.HBM, pl.ANY))
    n = len({v[3] for v in messages().values()})
    values, sums = ((2, 4, 2, 512, 128), jnp.bfloat16), ((2, 1024), jnp.float32)
    held = pl.pallas_call(
        kernel,
        out_shape=(pltpu.VMEM(*values), pltpu.VMEM(*sums)),
        in_specs=[hbm] * 6,
        scratch_shapes=[
            pltpu.SMEM((2, 4), jnp.int32),
            pltpu.SMEM((2,), jnp.int32),
            pltpu.SMEM((3, 16), jnp.int32),
            pltpu.VMEM((16, 128), jnp.float32),
            pltpu.VMEM((NZ, NY, 2, TILES, 8, 128), jnp.bfloat16),
            pltpu.VMEM((4, 2, 4, 2, 512, 128), jnp.bfloat16),
            pltpu.VMEM((2, 2, 4, 512, 128), jnp.bfloat16),
            pltpu.VMEM((4, 1536, 256), jnp.bfloat16),
            pltpu.VMEM((2, 2, 512, 128), jnp.float32),
            pltpu.VMEM((2, 2 * UNITS[-1][2], 256), jnp.float32),
            pltpu.VMEM((4, 2, 1024), jnp.float32),
            pltpu.VMEM((4, 2, 512 - TAIL), jnp.float32),
            pltpu.SemaphoreType.DMA((n,)),
            pltpu.SemaphoreType.DMA((1,)),
            pltpu.SemaphoreType.DMA((4,)),
            pltpu.SemaphoreType.DMA((4,)),
            pltpu.SemaphoreType.REGULAR,
        ],
        compiler_params=pltpu.CompilerParams(collective_id=0, has_side_effects=True, vmem_limit_bytes=VMEM_BYTES),
    )(slot_ids, slot_count, pattern.T, band_tiles.reshape(48, 8, 128), orbitals.reshape(2, 4, 2, 512, 128), occupation)
    rotated, density = pl.pallas_call(
        write_out,
        out_shape=(jax.ShapeDtypeStruct(*values), jax.ShapeDtypeStruct(*sums)),
        in_specs=[anywhere] * 2,
        out_specs=(hbm, hbm),
        scratch_shapes=[pltpu.SemaphoreType.DMA((9,))],
        compiler_params=pltpu.CompilerParams(vmem_limit_bytes=1024 * 1024),
    )(*held)
    return rotated.reshape(2, 4, 1024, 128), density


def solution(mesh):
    return jax.shard_map(
        local,
        mesh=mesh,
        in_specs=(
            P("dom", None, None, "orb"),
            P("dom", None),
            P("dom"),
            P(None, None, "dom", "orb"),
            P(),
            P(None, "orb"),
        ),
        out_specs=(P("dom", None, None, "orb"), P("dom", None)),
        check_vma=False,
    )
```

```python
import functools
import heapq

import jax
import jax.numpy as jnp
from jax import lax
from jax.experimental import pallas as pl
from jax.experimental.pallas import tpu as pltpu
from jax.sharding import PartitionSpec as P

MESH = pl.DeviceIdType.MESH
NX, NY, NZ = 4, 4, 8
TILES = 46
A_TILES = 18
VMEM_BYTES = 67043328 - 2097152 - 8192
B_SETS = {1: (0, 1, -2, 3), -1: (-1, 2, -3, 4)}
CHUNKS = [(0, 0, 256), (0, 256, 256), (1, 0, 128), (1, 128, 128), (1, 256, 128), (1, 384, 64), (1, 448, 48), (1, 496, 16)]
UNITS = [(0, 0, 256), (0, 256, 256), (1, 0, 256), (1, 256, 128), (1, 384, 64), (1, 448, 64)]
TAIL = 384
SHARED = 4
DIRECT = len(CHUNKS) - 1
DEPTH = 3
COMPUTE = (
    ("s1", "w", "p0", "s2", "p1", "s3", "p2", "s4", "s5", "p3", "s6", "p4", "d", "s7", "b5", "p5"),
    ("s1", "s2", "w", "p0", "s3", "p1", "s4", "s5", "s6", "p2", "p3", "p4", "d", "s7", "b5", "p5"),
)


def messages():
    tile = 8 * 128 * 2
    a, b = A_TILES * tile, (TILES - A_TILES) * tile
    out = {}

    def add(key, link, size, needs, group=None):
        out[key] = (link, size, needs, group or key)

    add(("swap",), "xs", a + b, [("tiles",)])
    half_of = {1: 0, -1: 1}
    mine = [[("z",)], [("z",), ("swap",)]]
    for n in range(1, 4):
        for w in range(2):
            for s in (1, -1):
                add(("Bz", s, n, w), ("z", s), b, mine[w] if n == 1 else [("Bz", n - 1, w)], ("Bz", n, w))
    for s in (1, -1):
        add(("Bz", s, 4, half_of[s]), ("z", s), b, [("Bz", 3, half_of[s])], ("Bz4",))
    for w in range(2):
        for s in (1, -1):
            add(("Ay1", s, w), ("y", s), a, mine[w], ("Ay1", w))
    for s in (1, -1):
        add(("Ay2", s, half_of[s]), ("y", s), a, [("Ay1", half_of[s])], ("Ay2",))
    sides = [("Ay1", 0), ("Ay1", 1)]
    have_a = {0: mine[1], -1: sides, 1: sides, 2: [("Ay2",)]}
    for dy in (0, -1, 1, 2):
        for n in range(1, 5):
            for s in (1, -1):
                before = [("Az", dy, n - 1)] if dy or n == 4 else [("Az", dy, n - 1, w) for w in range(2)]
                if n == 4:
                    add(("Az", s, dy, 4, half_of[s]), ("z", s), a, before, ("Az4",))
                elif dy == 0 and n < 3:
                    for w in range(2):
                        add(("Az", s, dy, n, w), ("z", s), a, mine[w] if n == 1 else [("Az", dy, n - 1, w)], ("Az", dy, n, w))
                else:
                    add(("Az", s, dy, n), ("z", s), 2 * a, have_a[dy] if n == 1 else before, ("Az", dy, n))
    have_b = {0: mine[1], 4: [("Bz4",)]}
    for n in range(1, 4):
        have_b[-n] = have_b[n] = [("Bz", n, 0), ("Bz", n, 1)]
    for dz in (0, -1, 1, -2, 2, -3, 3, 4):
        for s in (1, -1):
            onward = dz in B_SETS[s]
            group = ("By1", s, dz) if onward else ("By1", s)
            if dz == 0:
                for w in range(2):
                    add(("By1", s, dz, w), ("y", s), b, mine[w], group)
            else:
                add(("By1", s, dz), ("y", s), 2 * b, have_b[dz], group)
            if onward:
                add(("By2", s, dz), ("y", s), 2 * b, [("By1", s, dz)], ("By2",))
    row = 4 * 128 * 2
    for i in range(4):
        for s in (1, -1):
            add(("X1", s, i), ("x", s), 256 * row, [("own", i // 2)], ("X1", i))
    add(("Od",), "d", 2048 * row, [("own", 0), ("own", 1), ("z",)])
    for k, (g, first, rows) in enumerate(CHUNKS):
        for s in (1, -1):
            add(("X2", s, k), ("x", s), rows * row, [("X1", g * 2 + first // 256)], ("X2", k))
            if k == DIRECT:
                add(("X2c", s, k), ("x", s), rows * row, [("X1", g * 2 + first // 256)], ("X2", k))
        if k < DIRECT:
            add(("Xd", k), "d", 2 * rows * row, [("X2", k)])
    return out


def chunks_of(u):
    if u >= len(UNITS):
        return []
    g, first, rows = UNITS[u]
    return [k for k, (cg, ca, _) in enumerate(CHUNKS) if cg == g and first <= ca < first + rows]


def plan():
    todo = messages()
    rate = {"d": 690e3}
    left, after = {}, {}
    for key, (_, _, needs, group) in todo.items():
        left.setdefault(group, set()).add(key)
        for need in needs:
            after.setdefault(need, []).append(key)

    @functools.lru_cache(None)
    def path(key):
        link, size, _, group = todo[key]
        return size / rate.get(link, 46.9e3) + 1.9 + max([path(k) for k in after.get(group, [])], default=0)

    free, here, due, order, pending = {}, set(), [], [], dict(todo)
    now = 0.0

    def send_ready():
        ready = [k for k, v in pending.items() if all(need in here for need in v[2])]
        for key in sorted(ready, key=lambda k: -path(k) if k[0][0] in "AB" else 0):
            link, size, _, group = todo[key]
            busy = [t for t in free.get(link, []) if t > now]
            if link[0] in "yz" and len(busy) >= DEPTH:
                continue
            pending.pop(key)
            links = [("x", 1), ("x", -1)] if link == "xs" else [link]
            start = max([now] + [t for one in links for t in free.get(one, [])[-1:]])
            end = start + size / rate.get(link, 46.9e3)
            for one in links:
                free.setdefault(one, []).append(end)
            heapq.heappush(due, (end + (1.0 if link == "d" else 1.9), len(order), key))
            order.append(("send", key))

    for i, group in enumerate([("tiles",), ("own", 0), ("own", 1), ("z",)]):
        heapq.heappush(due, (0.5 if group == ("z",) else 0.01 * i, i - 50, group))
        left[group] = {group}
    first = {g for g in left if g[0] not in ("X2", "Xd", "Od")} | {("X2", 0)}
    while not first <= here:
        now = max(now, due[0][0])
        key = heapq.heappop(due)[2]
        group = todo[key][3] if key in todo else key
        left[group].discard(key)
        if left[group] or group not in first:
            continue
        order.append(("wait", group))
        here.add(group)
        send_ready()

    def forward(*chunks):
        return [step for k in chunks for step in [("wait", ("X2", k))] + [("send", ("Xd", k))] * (k < DIRECT)]

    def product(u):
        return [("wait", ("Xd", k)) for k in chunks_of(u) if k < DIRECT] + [("product", u)]

    def expand(steps):
        out = []
        for name in steps:
            kind, i = name[0], int(name[1:] or 0)
            if kind == "s":
                out += forward(i)
            elif kind == "p":
                out += [("wait", ("Od",))] * (i == 0) + product(i)
            else:
                out.append(({"w": "weights", "b": "begin", "d": "share"}[kind], i))
        return out

    return order, [expand(steps) for steps in COMPUTE]


def kernel(
    ids_in, count_in, pattern_in, band, orbitals, occ_in, rotated, density,
    ids, count, pattern, occ, T, X, F, W, D, E, dens, tails, recv, sent, local, shared, ready,
):
    dom, orb = lax.axis_index("dom"), lax.axis_index("orb")
    x_lo, z, y = lax.div(dom, 32), lax.rem(lax.div(dom, 4), 8), lax.rem(dom, 4)
    x_hi, core = lax.div(orb, 2), lax.rem(orb, 2)
    x = x_hi * 2 + x_lo

    def at_x(step):
        return lax.rem(x + step + NX, NX)

    def at_y(step):
        return lax.rem(y + step + NY, NY)

    def at_z(step):
        return lax.rem(z + step + NZ, NZ)

    def device(px, py, pz, pc):
        return (lax.rem(px, 2) * 32 + pz * 4 + py, lax.div(px, 2) * 2 + pc)

    far = lax.div(at_x(2), 2) * 2 + core
    to = {"xs": device(x + 1 - 2 * x_lo, y, z, core), "d": device(x, y, z, 1 - core)}
    for s in (1, -1):
        to["x", s] = device(at_x(s), y, z, core)
        to["y", s] = device(x, at_y(s), z, core)
        to["z", s] = device(x, y, at_z(s), core)

    A, B, BOTH, ALL = pl.ds(0, A_TILES), pl.ds(A_TILES, TILES - A_TILES), pl.ds(0, 2), slice(None)

    def low(w=None):
        return BOTH if w is None else pl.ds(x_lo + w - 2 * w * x_lo, 1)

    def side(s):
        return 0 if s > 0 else 1

    todo = messages()
    groups = list(dict.fromkeys(v[3] for v in todo.values()))
    number = {group: i for i, group in enumerate(groups)}

    def ends(key):
        kind = key[0]
        if kind == "swap":
            return (T.at[z, y, x_lo],) * 2
        if kind == "Bz":
            _, s, n, w = key
            return (T.at[at_z(-(n - 1) * s), y, low(w), B],) * 2
        if kind == "Ay1":
            return (T.at[z, y, low(key[2]), A],) * 2
        if kind == "Ay2":
            return (T.at[z, at_y(-key[1]), low(key[2]), A],) * 2
        if kind == "Az":
            s, dy, n = key[1:4]
            return (T.at[at_z(-(n - 1) * s), at_y(dy), low(*key[4:]), A],) * 2
        if kind == "By1":
            return (T.at[at_z(key[2]), y, low(*key[3:]), B],) * 2
        if kind == "By2":
            return (T.at[at_z(key[2]), at_y(-key[1]), BOTH, B],) * 2
        if kind == "X1":
            _, s, i = key
            rows = pl.ds(i % 2 * 256, 256)
            return X.at[orb, i // 2, ALL, side(s), rows], F.at[side(s), i // 2, ALL, rows]
        if kind in ("X2", "X2c"):
            _, s, k = key
            g, first, rows = CHUNKS[k]
            source = lax.div(at_x(-s), 2) * 2 + core
            return F.at[side(s), g, ALL, pl.ds(first, rows)], X.at[source, g, ALL, side(s), pl.ds(first, rows)]
        if kind == "Xd":
            g, first, rows = CHUNKS[key[1]]
            return (X.at[far, g, ALL, ALL, pl.ds(first, rows)],) * 2
        return (X.at[orb],) * 2

    def copy(key):
        src, dst = ends(key)
        return pltpu.make_async_remote_copy(
            src_ref=src, dst_ref=dst, send_sem=sent.at[0], recv_sem=recv.at[number[todo[key][3]]],
            device_id=device(at_x(key[1]), y, z, 1 - core) if key[0] == "X2c" else to[todo[key][0]], device_id_type=MESH,
        )

    def landed(group):
        kind = group[0]
        one, two = pl.ds(0, 1), pl.ds(0, 2)
        if kind == "Bz":
            where = T.at[two, y, one, B]
        elif kind == "Bz4":
            where = T.at[z, y, BOTH, B]
        elif kind == "Ay1":
            where = T.at[z, two, one, A]
        elif kind == "Ay2":
            where = T.at[z, y, BOTH, A]
        elif kind == "Az":
            where = T.at[two, y, BOTH if len(group) == 3 else one, A]
        elif kind == "Az4":
            where = T.at[z, ALL, BOTH, A]
        elif kind == "By1":
            where = T.at[z, y, BOTH, B] if len(group) == 3 else T.at[pl.ds(0, 4), y, BOTH, B]
        elif kind == "By2":
            where = T.at[ALL, y, BOTH, B]
        elif kind == "X1":
            where = F.at[ALL, group[1] // 2, ALL, pl.ds(group[1] % 2 * 256, 256)]
        elif kind == "X2":
            g, first, rows = CHUNKS[group[1]]
            orbs = pl.ds(lax.div(at_x(2), 2) * 2, 2) if group[1] == DIRECT else far
            where = X.at[orbs, g, ALL, ALL, pl.ds(first, rows)]
        else:
            where = ends(group)[1]
        pltpu.make_async_copy(where, where, recv.at[number[group]]).wait()

    loads = {("tiles",): pltpu.make_async_copy(band.at[pl.ds(1, TILES)], T.at[z, y, x_lo], local.at[0])}
    for g in range(2):
        loads["own", g] = pltpu.make_async_copy(orbitals.at[g], X.at[orb, g], local.at[1 + g])
    tables = [
        pltpu.make_async_copy(here, there, local.at[3])
        for here, there in ((ids_in, ids), (count_in, count), (pattern_in, pattern), (occ_in, occ))
    ]

    def weights():
        for g in range(2):
            for pair in range(2):
                for at in range(3):
                    l = pair + at
                    for half in range(2):
                        m = pair * 2 + half
                        columns = pl.ds(half * 128, 128)
                        if abs(l - m) > 1:
                            W[g * 2 + pair, pl.ds(at * 512, 512), columns] = jnp.zeros((512, 128), jnp.bfloat16)
                            continue
                        source, target = ids[g, l], ids[g, m]
                        column = target - source + 1
                        inside = (column >= 0) & (column < 3)
                        column = jnp.clip(column, 0, 2)
                        keep = inside & (pattern[column, source] == 1) & (max(l, m) < count[g])
                        t = jnp.clip(source * 3 + column - 1, 0, TILES - 1)
                        scale = jnp.where(keep, jnp.float32(1), jnp.float32(0))
                        for low in range(2):
                            rows = T[:, :, low, t].astype(jnp.float32).reshape(256, 128) * scale
                            W[g * 2 + pair, pl.ds(at * 512 + low * 256, 256), columns] = rows.astype(jnp.bfloat16)

    def lane_sums(u):
        g, first, n = UNITS[u]
        for half in range(2):
            total = D[g, half, pl.ds(first, n)]
            dens[orb, pl.ds(g, 1), pl.ds(half * 512 + first, n)] = jnp.sum(total.T, axis=0, keepdims=True)

    def multiply(u, pair, orbs):
        g, first, n = UNITS[u]
        parts = [(at, q) for at in range(3) for q in orbs]
        values = jnp.concatenate(
            [jnp.concatenate([X[q, g, pair + at, half, pl.ds(first, n)] for at, q in parts], axis=1) for half in range(2)], axis=0
        )
        if len(orbs) == 4:
            tiles = W[g * 2 + pair]
        else:
            tiles = jnp.concatenate([W[g * 2 + pair, pl.ds(pl.multiple_of(at * 512 + q * 128, 128), 128)] for at, q in parts], axis=0)
        return jnp.dot(values, tiles, preferred_element_type=jnp.float32)

    def begin(u):
        for pair in range(2):
            E[pair] = multiply(u, pair, (orb, x_hi * 2 + 1 - core, far))

    def product(u):
        g, first, n = UNITS[u]
        rows = pl.ds(first, n)
        total = jnp.zeros((2 * n, 128), jnp.float32)
        for pair in range(2):
            if u < len(UNITS) - 1:
                out = multiply(u, pair, range(4))
            else:
                out = E[pair] + multiply(u, pair, (lax.div(at_x(2), 2) * 2 + 1 - core,))
            out = out.astype(jnp.bfloat16)
            for which in range(2):
                m = pair * 2 + which
                one = out[:, which * 128 : which * 128 + 128]
                for half in range(2):
                    rotated[g, m, half, rows] = one[half * n : half * n + n]
                wide = one.astype(jnp.float32)
                total = total + wide * wide * occ[pl.ds(ids[g, m], 1), :]
        for half in range(2):
            D[g, half, rows] = total[half * n : half * n + n]
        if 1 <= u <= SHARED:
            lane_sums(u - 1)
        if u == len(UNITS) - 1:
            for half in range(2):
                tails[orb, pl.ds(half, 1)] = jnp.sum(D[1, half, pl.ds(TAIL, 512 - TAIL)].T, axis=0, keepdims=True)

    barrier = pltpu.get_barrier_semaphore()
    for step in (1, -1):
        pl.semaphore_signal(barrier, inc=1, device_id=to["x", step], device_id_type=MESH)
    for step in (1, -1):
        pl.semaphore_signal(barrier, inc=1, device_id=device(x, at_y(step), z, 0), device_id_type=MESH)
        pl.semaphore_signal(barrier, inc=1, device_id=device(x, y, at_z(step), 0), device_id_type=MESH)

    @pl.when(core == 1)
    def _():
        pl.semaphore_signal(barrier, inc=1, device_id=device(x, y, z, 0), device_id_type=MESH)

    for load in loads.values():
        load.start()
    for table in tables:
        table.start()

    @pl.when(core == 0)
    def _():
        pl.semaphore_wait(barrier, 11)
        pl.semaphore_signal(ready, inc=1, device_id=device(x, y, z, 1), device_id_type=MESH)

    @pl.when(core == 1)
    def _():
        pl.semaphore_wait(barrier, 2)

    def neighbours():
        @pl.when(core == 1)
        def _():
            pl.semaphore_wait(ready, 1)

    def share(sums, which):
        for peer in (device(at_x(2), y, z, core), device(at_x(2), y, z, 1 - core), to["d"]):
            pltpu.make_async_remote_copy(
                src_ref=sums.at[orb], dst_ref=sums.at[orb], send_sem=shared.at[2 * which], recv_sem=shared.at[2 * which + 1],
                device_id=peer, device_id_type=MESH,
            ).start()

    def shared_by_all(sums, which):
        for end in range(2):
            three = sums.at[pl.ds(0, 3)]
            pltpu.make_async_copy(three, three, shared.at[2 * which + end]).wait()

    def run(steps):
        for step in steps:
            if step[0] == "send":
                copy(step[1]).start()
            elif step[0] == "product":
                product(step[1])
            elif step[0] == "begin":
                begin(step[1])
            elif step[0] == "share":
                share(dens, 0)
            elif step[0] == "weights":
                for table in tables:
                    table.wait()
                weights()
            elif step[1] in loads:
                loads[step[1]].wait()
            elif step[1] == ("z",):
                neighbours()
            else:
                landed(step[1])

    order, by_core = plan()
    run(order)
    if by_core[0] == by_core[1]:
        run(by_core[0])
    else:
        for which in range(2):
            pl.when(core == which)(functools.partial(run, by_core[which]))

    share(tails, 1)
    shared_by_all(dens, 0)
    density[...] = dens[0] + dens[1] + dens[2] + dens[3]
    for key in todo:
        copy(key).wait_send()
    shared_by_all(tails, 1)
    last = tails[0] + tails[1] + tails[2] + tails[3]
    for half in range(2):
        density[1:2, pl.ds(half * 512 + TAIL, 512 - TAIL)] = last[half : half + 1]


def write_out(held, held_density, rotated, density, sem):
    copies = [pltpu.make_async_copy(held.at[g, m], rotated.at[g, m], sem.at[g * 4 + m]) for g in range(2) for m in range(4)]
    copies.append(pltpu.make_async_copy(held_density, density, sem.at[8]))
    for one in copies:
        one.start()
    for one in copies:
        one.wait()


def local(orbitals, slot_ids, slot_count, band_tiles, pattern, occupation):
    hbm, anywhere = (pl.BlockSpec(memory_space=s) for s in (pltpu.HBM, pl.ANY))
    n = len({v[3] for v in messages().values()})
    values, sums = ((2, 4, 2, 512, 128), jnp.bfloat16), ((2, 1024), jnp.float32)
    held = pl.pallas_call(
        kernel,
        out_shape=(pltpu.VMEM(*values), pltpu.VMEM(*sums)),
        in_specs=[hbm] * 6,
        scratch_shapes=[
            pltpu.SMEM((2, 4), jnp.int32),
            pltpu.SMEM((2,), jnp.int32),
            pltpu.SMEM((3, 16), jnp.int32),
            pltpu.VMEM((16, 128), jnp.float32),
            pltpu.VMEM((NZ, NY, 2, TILES, 8, 128), jnp.bfloat16),
            pltpu.VMEM((4, 2, 4, 2, 512, 128), jnp.bfloat16),
            pltpu.VMEM((2, 2, 4, 512, 128), jnp.bfloat16),
            pltpu.VMEM((4, 1536, 256), jnp.bfloat16),
            pltpu.VMEM((2, 2, 512, 128), jnp.float32),
            pltpu.VMEM((2, 2 * UNITS[-1][2], 256), jnp.float32),
            pltpu.VMEM((4, 2, 1024), jnp.float32),
            pltpu.VMEM((4, 2, 512 - TAIL), jnp.float32),
            pltpu.SemaphoreType.DMA((n,)),
            pltpu.SemaphoreType.DMA((1,)),
            pltpu.SemaphoreType.DMA((4,)),
            pltpu.SemaphoreType.DMA((4,)),
            pltpu.SemaphoreType.REGULAR,
        ],
        compiler_params=pltpu.CompilerParams(collective_id=0, has_side_effects=True, vmem_limit_bytes=VMEM_BYTES),
    )(slot_ids, slot_count, pattern.T, band_tiles.reshape(48, 8, 128), orbitals.reshape(2, 4, 2, 512, 128), occupation)
    rotated, density = pl.pallas_call(
        write_out,
        out_shape=(jax.ShapeDtypeStruct(*values), jax.ShapeDtypeStruct(*sums)),
        in_specs=[anywhere] * 2,
        out_specs=(hbm, hbm),
        scratch_shapes=[pltpu.SemaphoreType.DMA((9,))],
        compiler_params=pltpu.CompilerParams(vmem_limit_bytes=1024 * 1024),
    )(*held)
    return rotated.reshape(2, 4, 1024, 128), density


def solution(mesh):
    return jax.shard_map(
        local,
        mesh=mesh,
        in_specs=(
            P("dom", None, None, "orb"),
            P("dom", None),
            P("dom"),
            P(None, None, "dom", "orb"),
            P(),
            P(None, "orb"),
        ),
        out_specs=(P("dom", None, None, "orb"), P("dom", None)),
        check_vma=False,
    )
```

```python
import functools
import heapq

import jax
import jax.numpy as jnp
from jax import lax
from jax.experimental import pallas as pl
from jax.experimental.pallas import tpu as pltpu
from jax.sharding import PartitionSpec as P

MESH = pl.DeviceIdType.MESH
NX, NY, NZ = 4, 4, 8
TILES = 46
A_TILES = 18
VMEM_BYTES = 67043328 - 2097152 - 8192
B_SETS = {1: (0, 1, -2, 3), -1: (-1, 2, -3, 4)}
CHUNKS = [(0, 0, 256), (0, 256, 256), (1, 0, 128), (1, 128, 128), (1, 256, 128), (1, 384, 64), (1, 448, 64)]
UNITS = [(0, 0, 256), (0, 256, 256), (1, 0, 256), (1, 256, 128), (1, 384, 64), (1, 448, 64)]
TAIL = 384
SHARED = 4
DIRECT = len(CHUNKS)
DEPTH = 3
COMPUTE = (
    ("s1", "w", "p0", "s2", "p1", "s3", "p2", "s4", "s5", "p3", "s6", "p4", "d", "b5", "p5"),
    ("s1", "s2", "w", "p0", "s3", "p1", "s4", "s5", "s6", "p2", "p3", "p4", "d", "b5", "p5"),
)


def messages():
    tile = 8 * 128 * 2
    a, b = A_TILES * tile, (TILES - A_TILES) * tile
    out = {}

    def add(key, link, size, needs, group=None):
        out[key] = (link, size, needs, group or key)

    add(("swap",), "xs", a + b, [("tiles",)])
    half_of = {1: 0, -1: 1}
    mine = [[("z",)], [("z",), ("swap",)]]
    for n in range(1, 4):
        for w in range(2):
            for s in (1, -1):
                add(("Bz", s, n, w), ("z", s), b, mine[w] if n == 1 else [("Bz", n - 1, w)], ("Bz", n, w))
    for s in (1, -1):
        add(("Bz", s, 4, half_of[s]), ("z", s), b, [("Bz", 3, half_of[s])], ("Bz4",))
    for w in range(2):
        for s in (1, -1):
            add(("Ay1", s, w), ("y", s), a, mine[w], ("Ay1", w))
    for s in (1, -1):
        add(("Ay2", s, half_of[s]), ("y", s), a, [("Ay1", half_of[s])], ("Ay2",))
    sides = [("Ay1", 0), ("Ay1", 1)]
    have_a = {0: mine[1], -1: sides, 1: sides, 2: [("Ay2",)]}
    for dy in (0, -1, 1, 2):
        for n in range(1, 5):
            for s in (1, -1):
                before = [("Az", dy, n - 1)] if dy or n == 4 else [("Az", dy, n - 1, w) for w in range(2)]
                if n == 4:
                    add(("Az", s, dy, 4, half_of[s]), ("z", s), a, before, ("Az4",))
                elif dy == 0 and n < 3:
                    for w in range(2):
                        add(("Az", s, dy, n, w), ("z", s), a, mine[w] if n == 1 else [("Az", dy, n - 1, w)], ("Az", dy, n, w))
                else:
                    add(("Az", s, dy, n), ("z", s), 2 * a, have_a[dy] if n == 1 else before, ("Az", dy, n))
    have_b = {0: mine[1], 4: [("Bz4",)]}
    for n in range(1, 4):
        have_b[-n] = have_b[n] = [("Bz", n, 0), ("Bz", n, 1)]
    for dz in (0, -1, 1, -2, 2, -3, 3, 4):
        for s in (1, -1):
            onward = dz in B_SETS[s]
            group = ("By1", s, dz) if onward else ("By1", s)
            if dz == 0:
                for w in range(2):
                    add(("By1", s, dz, w), ("y", s), b, mine[w], group)
            else:
                add(("By1", s, dz), ("y", s), 2 * b, have_b[dz], group)
            if onward:
                add(("By2", s, dz), ("y", s), 2 * b, [("By1", s, dz)], ("By2",))
    row = 4 * 128 * 2
    for i in range(2):
        for s in (1, -1):
            add(("X1", s, i), ("x", s), 512 * row, [("own", i)], ("X1", i))
    add(("Od",), "d", 2048 * row, [("own", 0), ("own", 1), ("z",)])
    for k, (g, first, rows) in enumerate(CHUNKS):
        for s in (1, -1):
            add(("X2", s, k), ("x", s), rows * row, [("X1", g)], ("X2", k))
            if k == DIRECT:
                add(("X2c", s, k), ("x", s), rows * row, [("X1", g)], ("X2", k))
        if k < DIRECT:
            add(("Xd", k), "d", 2 * rows * row, [("X2", k)])
    return out


def chunks_of(u):
    if u >= len(UNITS):
        return []
    g, first, rows = UNITS[u]
    return [k for k, (cg, ca, _) in enumerate(CHUNKS) if cg == g and first <= ca < first + rows]


def plan():
    todo = messages()
    rate = {"d": 690e3}
    left, after = {}, {}
    for key, (_, _, needs, group) in todo.items():
        left.setdefault(group, set()).add(key)
        for need in needs:
            after.setdefault(need, []).append(key)

    @functools.lru_cache(None)
    def path(key):
        link, size, _, group = todo[key]
        return size / rate.get(link, 46.9e3) + 1.9 + max([path(k) for k in after.get(group, [])], default=0)

    free, here, due, order, pending = {}, set(), [], [], dict(todo)
    now = 0.0

    def send_ready():
        ready = [k for k, v in pending.items() if all(need in here for need in v[2])]
        for key in sorted(ready, key=lambda k: -path(k) if k[0][0] in "AB" else 0):
            link, size, _, group = todo[key]
            busy = [t for t in free.get(link, []) if t > now]
            if link[0] in "yz" and len(busy) >= DEPTH:
                continue
            pending.pop(key)
            links = [("x", 1), ("x", -1)] if link == "xs" else [link]
            start = max([now] + [t for one in links for t in free.get(one, [])[-1:]])
            end = start + size / rate.get(link, 46.9e3)
            for one in links:
                free.setdefault(one, []).append(end)
            heapq.heappush(due, (end + (1.0 if link == "d" else 1.9), len(order), key))
            order.append(("send", key))

    for i, group in enumerate([("tiles",), ("own", 0), ("own", 1), ("z",)]):
        heapq.heappush(due, (0.5 if group == ("z",) else 0.01 * i, i - 50, group))
        left[group] = {group}
    first = {g for g in left if g[0] not in ("X2", "Xd", "Od")} | {("X2", 0)}
    while not first <= here:
        now = max(now, due[0][0])
        key = heapq.heappop(due)[2]
        group = todo[key][3] if key in todo else key
        left[group].discard(key)
        if left[group] or group not in first:
            continue
        order.append(("wait", group))
        here.add(group)
        send_ready()

    def forward(*chunks):
        return [step for k in chunks for step in [("wait", ("X2", k))] + [("send", ("Xd", k))] * (k < DIRECT)]

    def product(u):
        return [("wait", ("Xd", k)) for k in chunks_of(u) if k < DIRECT] + [("product", u)]

    def expand(steps):
        out = []
        for name in steps:
            kind, i = name[0], int(name[1:] or 0)
            if kind == "s":
                out += forward(i)
            elif kind == "p":
                out += [("wait", ("Od",))] * (i == 0) + product(i)
            else:
                out.append(({"w": "weights", "b": "begin", "d": "share"}[kind], i))
        return out

    return order, [expand(steps) for steps in COMPUTE]


def kernel(
    ids_in, count_in, pattern_in, band, orbitals, occ_in, rotated, density,
    ids, count, pattern, occ, T, X, F, W, D, E, dens, tails, recv, sent, local, shared, ready,
):
    dom, orb = lax.axis_index("dom"), lax.axis_index("orb")
    x_lo, z, y = lax.div(dom, 32), lax.rem(lax.div(dom, 4), 8), lax.rem(dom, 4)
    x_hi, core = lax.div(orb, 2), lax.rem(orb, 2)
    x = x_hi * 2 + x_lo

    def at_x(step):
        return lax.rem(x + step + NX, NX)

    def at_y(step):
        return lax.rem(y + step + NY, NY)

    def at_z(step):
        return lax.rem(z + step + NZ, NZ)

    def device(px, py, pz, pc):
        return (lax.rem(px, 2) * 32 + pz * 4 + py, lax.div(px, 2) * 2 + pc)

    far = lax.div(at_x(2), 2) * 2 + core
    to = {"xs": device(x + 1 - 2 * x_lo, y, z, core), "d": device(x, y, z, 1 - core)}
    for s in (1, -1):
        to["x", s] = device(at_x(s), y, z, core)
        to["y", s] = device(x, at_y(s), z, core)
        to["z", s] = device(x, y, at_z(s), core)

    A, B, BOTH, ALL = pl.ds(0, A_TILES), pl.ds(A_TILES, TILES - A_TILES), pl.ds(0, 2), slice(None)

    def low(w=None):
        return BOTH if w is None else pl.ds(x_lo + w - 2 * w * x_lo, 1)

    def side(s):
        return 0 if s > 0 else 1

    todo = messages()
    groups = list(dict.fromkeys(v[3] for v in todo.values()))
    number = {group: i for i, group in enumerate(groups)}

    def ends(key):
        kind = key[0]
        if kind == "swap":
            return (T.at[z, y, x_lo],) * 2
        if kind == "Bz":
            _, s, n, w = key
            return (T.at[at_z(-(n - 1) * s), y, low(w), B],) * 2
        if kind == "Ay1":
            return (T.at[z, y, low(key[2]), A],) * 2
        if kind == "Ay2":
            return (T.at[z, at_y(-key[1]), low(key[2]), A],) * 2
        if kind == "Az":
            s, dy, n = key[1:4]
            return (T.at[at_z(-(n - 1) * s), at_y(dy), low(*key[4:]), A],) * 2
        if kind == "By1":
            return (T.at[at_z(key[2]), y, low(*key[3:]), B],) * 2
        if kind == "By2":
            return (T.at[at_z(key[2]), at_y(-key[1]), BOTH, B],) * 2
        if kind == "X1":
            _, s, i = key
            return X.at[orb, i, ALL, side(s)], F.at[side(s), i]
        if kind in ("X2", "X2c"):
            _, s, k = key
            g, first, rows = CHUNKS[k]
            source = lax.div(at_x(-s), 2) * 2 + core
            return F.at[side(s), g, ALL, pl.ds(first, rows)], X.at[source, g, ALL, side(s), pl.ds(first, rows)]
        if kind == "Xd":
            g, first, rows = CHUNKS[key[1]]
            return (X.at[far, g, ALL, ALL, pl.ds(first, rows)],) * 2
        return (X.at[orb],) * 2

    def copy(key):
        src, dst = ends(key)
        return pltpu.make_async_remote_copy(
            src_ref=src, dst_ref=dst, send_sem=sent.at[0], recv_sem=recv.at[number[todo[key][3]]],
            device_id=device(at_x(key[1]), y, z, 1 - core) if key[0] == "X2c" else to[todo[key][0]], device_id_type=MESH,
        )

    def landed(group):
        kind = group[0]
        one, two = pl.ds(0, 1), pl.ds(0, 2)
        if kind == "Bz":
            where = T.at[two, y, one, B]
        elif kind == "Bz4":
            where = T.at[z, y, BOTH, B]
        elif kind == "Ay1":
            where = T.at[z, two, one, A]
        elif kind == "Ay2":
            where = T.at[z, y, BOTH, A]
        elif kind == "Az":
            where = T.at[two, y, BOTH if len(group) == 3 else one, A]
        elif kind == "Az4":
            where = T.at[z, ALL, BOTH, A]
        elif kind == "By1":
            where = T.at[z, y, BOTH, B] if len(group) == 3 else T.at[pl.ds(0, 4), y, BOTH, B]
        elif kind == "By2":
            where = T.at[ALL, y, BOTH, B]
        elif kind == "X1":
            where = F.at[ALL, group[1]]
        elif kind == "X2":
            g, first, rows = CHUNKS[group[1]]
            orbs = pl.ds(lax.div(at_x(2), 2) * 2, 2) if group[1] == DIRECT else far
            where = X.at[orbs, g, ALL, ALL, pl.ds(first, rows)]
        else:
            where = ends(group)[1]
        pltpu.make_async_copy(where, where, recv.at[number[group]]).wait()

    loads = {("tiles",): pltpu.make_async_copy(band.at[pl.ds(1, TILES)], T.at[z, y, x_lo], local.at[0])}
    for g in range(2):
        loads["own", g] = pltpu.make_async_copy(orbitals.at[g], X.at[orb, g], local.at[1 + g])
    tables = [
        pltpu.make_async_copy(here, there, local.at[3])
        for here, there in ((ids_in, ids), (count_in, count), (pattern_in, pattern), (occ_in, occ))
    ]

    def weights():
        for g in range(2):
            for pair in range(2):
                for at in range(3):
                    l = pair + at
                    for half in range(2):
                        m = pair * 2 + half
                        columns = pl.ds(half * 128, 128)
                        if abs(l - m) > 1:
                            W[g * 2 + pair, pl.ds(at * 512, 512), columns] = jnp.zeros((512, 128), jnp.bfloat16)
                            continue
                        source, target = ids[g, l], ids[g, m]
                        column = target - source + 1
                        inside = (column >= 0) & (column < 3)
                        column = jnp.clip(column, 0, 2)
                        keep = inside & (pattern[column, source] == 1) & (max(l, m) < count[g])
                        t = jnp.clip(source * 3 + column - 1, 0, TILES - 1)
                        scale = jnp.where(keep, jnp.float32(1), jnp.float32(0))
                        for low in range(2):
                            rows = T[:, :, low, t].astype(jnp.float32).reshape(256, 128) * scale
                            W[g * 2 + pair, pl.ds(at * 512 + low * 256, 256), columns] = rows.astype(jnp.bfloat16)

    def lane_sums(u):
        g, first, n = UNITS[u]
        for half in range(2):
            total = D[g, half, pl.ds(first, n)]
            dens[orb, pl.ds(g, 1), pl.ds(half * 512 + first, n)] = jnp.sum(total.T, axis=0, keepdims=True)

    def multiply(u, pair, orbs):
        g, first, n = UNITS[u]
        parts = [(at, q) for at in range(3) for q in orbs]
        values = jnp.concatenate(
            [jnp.concatenate([X[q, g, pair + at, half, pl.ds(first, n)] for at, q in parts], axis=1) for half in range(2)], axis=0
        )
        if len(orbs) == 4:
            tiles = W[g * 2 + pair]
        else:
            tiles = jnp.concatenate([W[g * 2 + pair, pl.ds(pl.multiple_of(at * 512 + q * 128, 128), 128)] for at, q in parts], axis=0)
        return jnp.dot(values, tiles, preferred_element_type=jnp.float32)

    def begin(u):
        for pair in range(2):
            E[pair] = multiply(u, pair, (orb, x_hi * 2 + 1 - core, far))

    def product(u):
        g, first, n = UNITS[u]
        rows = pl.ds(first, n)
        total = jnp.zeros((2 * n, 128), jnp.float32)
        for pair in range(2):
            if u < len(UNITS) - 1:
                out = multiply(u, pair, range(4))
            else:
                out = E[pair] + multiply(u, pair, (lax.div(at_x(2), 2) * 2 + 1 - core,))
            out = out.astype(jnp.bfloat16)
            for which in range(2):
                m = pair * 2 + which
                one = out[:, which * 128 : which * 128 + 128]
                for half in range(2):
                    rotated[g, m, half, rows] = one[half * n : half * n + n]
                wide = one.astype(jnp.float32)
                total = total + wide * wide * occ[pl.ds(ids[g, m], 1), :]
        for half in range(2):
            D[g, half, rows] = total[half * n : half * n + n]
        if 1 <= u <= SHARED:
            lane_sums(u - 1)
        if u == len(UNITS) - 1:
            for half in range(2):
                tails[orb, pl.ds(half, 1)] = jnp.sum(D[1, half, pl.ds(TAIL, 512 - TAIL)].T, axis=0, keepdims=True)

    barrier = pltpu.get_barrier_semaphore()
    for step in (1, -1):
        pl.semaphore_signal(barrier, inc=1, device_id=to["x", step], device_id_type=MESH)
    for step in (1, -1):
        pl.semaphore_signal(barrier, inc=1, device_id=device(x, at_y(step), z, 0), device_id_type=MESH)
        pl.semaphore_signal(barrier, inc=1, device_id=device(x, y, at_z(step), 0), device_id_type=MESH)

    @pl.when(core == 1)
    def _():
        pl.semaphore_signal(barrier, inc=1, device_id=device(x, y, z, 0), device_id_type=MESH)

    for load in loads.values():
        load.start()
    for table in tables:
        table.start()

    @pl.when(core == 0)
    def _():
        pl.semaphore_wait(barrier, 11)
        pl.semaphore_signal(ready, inc=1, device_id=device(x, y, z, 1), device_id_type=MESH)

    @pl.when(core == 1)
    def _():
        pl.semaphore_wait(barrier, 2)

    def neighbours():
        @pl.when(core == 1)
        def _():
            pl.semaphore_wait(ready, 1)

    def share(sums, which):
        for peer in (device(at_x(2), y, z, core), device(at_x(2), y, z, 1 - core), to["d"]):
            pltpu.make_async_remote_copy(
                src_ref=sums.at[orb], dst_ref=sums.at[orb], send_sem=shared.at[2 * which], recv_sem=shared.at[2 * which + 1],
                device_id=peer, device_id_type=MESH,
            ).start()

    def shared_by_all(sums, which):
        for end in range(2):
            three = sums.at[pl.ds(0, 3)]
            pltpu.make_async_copy(three, three, shared.at[2 * which + end]).wait()

    def run(steps):
        for step in steps:
            if step[0] == "send":
                copy(step[1]).start()
            elif step[0] == "product":
                product(step[1])
            elif step[0] == "begin":
                begin(step[1])
            elif step[0] == "share":
                share(dens, 0)
            elif step[0] == "weights":
                for table in tables:
                    table.wait()
                weights()
            elif step[1] in loads:
                loads[step[1]].wait()
            elif step[1] == ("z",):
                neighbours()
            else:
                landed(step[1])

    order, by_core = plan()
    run(order)
    if by_core[0] == by_core[1]:
        run(by_core[0])
    else:
        for which in range(2):
            pl.when(core == which)(functools.partial(run, by_core[which]))

    share(tails, 1)
    shared_by_all(dens, 0)
    density[...] = dens[0] + dens[1] + dens[2] + dens[3]
    for key in todo:
        copy(key).wait_send()
    shared_by_all(tails, 1)
    last = tails[0] + tails[1] + tails[2] + tails[3]
    for half in range(2):
        density[1:2, pl.ds(half * 512 + TAIL, 512 - TAIL)] = last[half : half + 1]


def write_out(held, held_density, rotated, density, sem):
    copies = [pltpu.make_async_copy(held.at[g, m], rotated.at[g, m], sem.at[g * 4 + m]) for g in range(2) for m in range(4)]
    copies.append(pltpu.make_async_copy(held_density, density, sem.at[8]))
    for one in copies:
        one.start()
    for one in copies:
        one.wait()


def local(orbitals, slot_ids, slot_count, band_tiles, pattern, occupation):
    hbm, anywhere = (pl.BlockSpec(memory_space=s) for s in (pltpu.HBM, pl.ANY))
    n = len({v[3] for v in messages().values()})
    values, sums = ((2, 4, 2, 512, 128), jnp.bfloat16), ((2, 1024), jnp.float32)
    held = pl.pallas_call(
        kernel,
        out_shape=(pltpu.VMEM(*values), pltpu.VMEM(*sums)),
        in_specs=[hbm] * 6,
        scratch_shapes=[
            pltpu.SMEM((2, 4), jnp.int32),
            pltpu.SMEM((2,), jnp.int32),
            pltpu.SMEM((3, 16), jnp.int32),
            pltpu.VMEM((16, 128), jnp.float32),
            pltpu.VMEM((NZ, NY, 2, TILES, 8, 128), jnp.bfloat16),
            pltpu.VMEM((4, 2, 4, 2, 512, 128), jnp.bfloat16),
            pltpu.VMEM((2, 2, 4, 512, 128), jnp.bfloat16),
            pltpu.VMEM((4, 1536, 256), jnp.bfloat16),
            pltpu.VMEM((2, 2, 512, 128), jnp.float32),
            pltpu.VMEM((2, 2 * UNITS[-1][2], 256), jnp.float32),
            pltpu.VMEM((4, 2, 1024), jnp.float32),
            pltpu.VMEM((4, 2, 512 - TAIL), jnp.float32),
            pltpu.SemaphoreType.DMA((n,)),
            pltpu.SemaphoreType.DMA((1,)),
            pltpu.SemaphoreType.DMA((4,)),
            pltpu.SemaphoreType.DMA((4,)),
            pltpu.SemaphoreType.REGULAR,
        ],
        compiler_params=pltpu.CompilerParams(collective_id=0, has_side_effects=True, vmem_limit_bytes=VMEM_BYTES),
    )(slot_ids, slot_count, pattern.T, band_tiles.reshape(48, 8, 128), orbitals.reshape(2, 4, 2, 512, 128), occupation)
    rotated, density = pl.pallas_call(
        write_out,
        out_shape=(jax.ShapeDtypeStruct(*values), jax.ShapeDtypeStruct(*sums)),
        in_specs=[anywhere] * 2,
        out_specs=(hbm, hbm),
        scratch_shapes=[pltpu.SemaphoreType.DMA((9,))],
        compiler_params=pltpu.CompilerParams(vmem_limit_bytes=1024 * 1024),
    )(*held)
    return rotated.reshape(2, 4, 1024, 128), density


def solution(mesh):
    return jax.shard_map(
        local,
        mesh=mesh,
        in_specs=(
            P("dom", None, None, "orb"),
            P("dom", None),
            P("dom"),
            P(None, None, "dom", "orb"),
            P(),
            P(None, "orb"),
        ),
        out_specs=(P("dom", None, None, "orb"), P("dom", None)),
        check_vma=False,
    )
```
